32 devices in a mesh: gx: 4 (over z), gy: 8 (over y, x, core).
Axes of the slice: x: 2, y: 2, z: 4, core: 2. Of those that a mesh axis runs over, the one named last changes fastest.
Arguments:
- coordinates: float32 [3, 65536], P(None, ('gx', 'gy')), may hold values from 0 to 1
- rhs: float32 [16, 65536], P(None, ('gx', 'gy')), may hold values from -70 to 70
- leaf_order: int32 [32, 2048], P(('gx', 'gy')), may hold values from 0 to 2047, each once within a row
- leaf_sizes: int32 [32], P(('gx', 'gy')), may hold values from 1 to 2048, 49152 in all
- inverse_scales: float32 [3], replicated, may hold values from 12 to 30
- noise_var: float32 [1], replicated, may hold values from 0.3 to 1
- u_factors: float32 [5, 64, 65536], P(None, None, ('gx', 'gy')), may hold values from -0.375 to 0.375
- v_factors: float32 [5, 64, 65536], P(None, None, ('gx', 'gy')), may hold values from -1 to 1
Outputs:
- solution: float32 [16, 65536], P(None, ('gx', 'gy'))
The draws below stay inside these ranges and needn't reach their ends.
Inputs may be any that keep to these rules, and one draw needn't show every extreme that they name: `leaf_sizes`: each leaf's live points stand first in leaf order.
All inputs are finite; a program needn't handle non-finite values. No bound on the sum of `leaf_sizes` on one device may be relied on, other than what follows from the above.
Results may differ from the reference program's by a relative error of at most 0.0001.
Values sent between devices are 32-bit elements; how exact they have to be, the bound alone decides.
No kernel may reach another device: no remote copies, remote signals or barrier semaphores. Data moves between devices by JAX's collectives and lax.ppermute only.
A program may use at most 128 MiB of HBM per device.

```python
import math
import jax
import jax.numpy as jnp
import numpy as np
from jax import lax

LEAF = 2048
RANK = 64
VECTORS = 16
ITERS = 3
LEVELS = 5
LEAVES = 32
POINTS = 65536


def draw_v_factors(key, part):
    key_values = jax.random.fold_in(key, 11)
    level_ids = jnp.arange(LEVELS, dtype=jnp.float32)
    level_scale = 1.0 / jnp.sqrt(LEAF * 2.0 ** level_ids)
    values = jnp.clip(jax.random.normal(key_values, (LEVELS, RANK, POINTS), jnp.float32), -5.0, 5.0)
    return values * level_scale[:, None, None]


def draw_rhs(key, part):
    key_main = jax.random.fold_in(key, 21)
    key_column = jax.random.fold_in(key, 22)
    key_row = jax.random.fold_in(key, 23)
    position = jnp.arange(POINTS, dtype=jnp.float32) / POINTS
    column_scale = jnp.exp(jax.random.uniform(key_column, (1, POINTS), jnp.float32, 0.0, math.log(2.5)))
    row_scale = jnp.exp(jax.random.uniform(key_row, (VECTORS, 1), jnp.float32, math.log(1.0 / 3.0), math.log(10.0 / 3.0)))
    base = jnp.clip(jax.random.normal(key_main, (VECTORS, POINTS), jnp.float32), -4.0, 4.0)
    base = base * 0.5 * jnp.exp(math.log(3.0) * position)[None, :]
    return base * column_scale * row_scale


def levels(rng, shape, shards, low, high):
    def one(dim, parts):
        draws = jax.random.uniform(jax.random.fold_in(jax.random.fold_in(rng, 6), dim), (parts,), jnp.float32, low / len(shards), high / len(shards))
        return jnp.repeat(jnp.exp(draws), shape[dim] // parts).reshape((-1,) + (1,) * (len(shape) - dim - 1))

    gain = one(*shards[0])
    for cut in shards[1:]:
        gain = gain * one(*cut)
    return gain


def profile(amount, total, bound, slope):
    weights = [(1 << 20) // math.isqrt(rank ** slope) + 1 for rank in range(2, amount + 1)]
    rest, counts = total - bound - (amount - 1), [1] * (amount - 1)
    while rest > 0:
        movable = [i for i in range(amount - 1) if counts[i] < bound]
        whole, left = sum([weights[i] for i in movable]), rest
        for i in movable:
            addition = min(bound - counts[i], max(1, left * weights[i] // whole), rest)
            counts[i] = counts[i] + addition
            rest = rest - addition
    return np.array([bound] + counts)


def ragged_sizes(stream_key, amount, total, reach, skew):
    if amount == 2:
        one = jax.random.randint(stream_key, (), max(1, total - reach), min(reach, total - 1) + 1)
        return jnp.stack([one, total - one])
    sizes = jnp.asarray(profile(amount, total, reach, skew), jnp.int32)
    couples = (amount - 1) // 2
    donor, taker = sizes[1:1 + 2 * couples:2], sizes[2:2 + 2 * couples:2]
    room = jnp.minimum(donor - 1, reach - taker)
    shifted = jax.random.randint(jax.random.fold_in(stream_key, 1), (couples,), 0, 1 << 20) % (room + 1)
    sizes = sizes.at[1:1 + 2 * couples:2].set(donor - shifted).at[2:2 + 2 * couples:2].set(taker + shifted)
    return sizes[jax.random.permutation(jax.random.fold_in(stream_key, 2), amount)]


def scatter_about(rng, extent, width, bound, cuts=(), kind=jnp.bfloat16):
    values = jax.random.normal(rng, extent, jnp.float32) * width
    if len(cuts) > 0:
        values = levels(rng, extent, cuts, -0.22, 0.18) * values
    return jnp.clip(values, min=-bound, max=bound).astype(kind)


def setup_inputs(seed: int = 0) -> dict:
    splits = jax.random.split(jax.random.key(seed), 9)
    return {
        "coordinates": jnp.clip(1.0 * jax.random.uniform(splits[0], (3, POINTS), jnp.float32) ** levels(splits[0], (3, POINTS), ((1, 32),), -0.2, 0.2), 0.0, 1.0),
        "rhs": draw_rhs(jax.random.fold_in(splits[8], 71), 0),
        "leaf_order": jax.vmap(lambda own: jax.random.permutation(own, LEAF))(jax.random.split(splits[2], LEAVES)).reshape((LEAVES, LEAF)).astype(jnp.int32),
        "leaf_sizes": ragged_sizes(splits[3], LEAVES, LEAVES * LEAF * 3 // 4, LEAF, 1).astype(jnp.int32),
        "inverse_scales": jnp.clip(jnp.exp(jax.random.uniform(splits[4], (3,), jnp.float32, math.log(12.0), math.log(30.0))), 12.0, 30.0),
        "noise_var": jnp.clip(jnp.exp(jax.random.uniform(splits[5], (1,), jnp.float32, math.log(0.3), math.log(1.0))), 0.3, 1.0),
        "u_factors": scatter_about(splits[6], (LEVELS, RANK, POINTS), (4 * RANK) ** -0.5, 0.375, ((2, 32),), jnp.float32),
        "v_factors": draw_v_factors(jax.random.fold_in(splits[8], 71), 0),
    }


epsilon = 1e-06
sqrt_three = math.sqrt(3.0)
highest = lax.Precision.HIGHEST

def build_kernel(scaled):
    width_all = scaled.shape[1]
    block_rows = min(512, width_all)
    pieces = []
    for start_row in range(0, width_all, block_rows):
        row_points = scaled[:, start_row:start_row + block_rows]
        differ = row_points[:, :, None] - scaled[:, None, :]
        distance = jnp.sqrt(lax.optimization_barrier(jnp.sum(differ * differ, axis=0)))
        pieces.append((1.0 + sqrt_three * distance) * jnp.exp(-sqrt_three * distance))
    return jnp.concatenate(pieces, axis=0)

def least_squares(columns, beta):
    count_cols = len(columns)
    cosines = []
    sines = []
    target = [beta] + [jnp.zeros_like(beta)] * count_cols
    upper = []
    for column_idx in range(count_cols):
        entries = list(columns[column_idx])
        for row_idx in range(column_idx):
            first_val = entries[row_idx]
            second_val = entries[row_idx + 1]
            entries[row_idx] = cosines[row_idx] * first_val + sines[row_idx] * second_val
            entries[row_idx + 1] = -sines[row_idx] * first_val + cosines[row_idx] * second_val
        first_val = entries[column_idx]
        second_val = entries[column_idx + 1]
        radius = jnp.sqrt(first_val * first_val + second_val * second_val)
        cosines.append(first_val / radius)
        sines.append(second_val / radius)
        entries[column_idx] = radius
        carried = target[column_idx]
        target[column_idx] = cosines[column_idx] * carried
        target[column_idx + 1] = -sines[column_idx] * carried
        upper.append(entries[:column_idx + 1])
    weights = [None] * count_cols
    for column_idx in reversed(range(count_cols)):
        accum = target[column_idx]
        for later_idx in range(column_idx + 1, count_cols):
            accum = accum - upper[later_idx][column_idx] * weights[later_idx]
        weights[column_idx] = accum / upper[column_idx][column_idx]
    return weights

def reference(coordinates, rhs, leaf_order, leaf_sizes, inverse_scales, noise_var, u_factors, v_factors):
    num_leaves = leaf_order.shape[0]
    leaf_len = leaf_order.shape[1]
    num_vectors = rhs.shape[0]
    num_levels = u_factors.shape[0]
    num_rank = u_factors.shape[1]
    num_points = num_leaves * leaf_len
    points = jnp.take_along_axis(coordinates.reshape(3, num_leaves, leaf_len), leaf_order[None], axis=2)
    scaled = points * inverse_scales[:, None, None]
    ordered = jnp.take_along_axis(rhs.reshape(num_vectors, num_leaves, leaf_len), leaf_order[None], axis=2)
    live_mask = (jnp.arange(leaf_len, dtype=jnp.int32)[None, :] < leaf_sizes[:, None]).astype(jnp.float32)
    scaled_leaves = jnp.moveaxis(scaled, 1, 0)

    def dense_part(vector):

        def one_leaf(pair):
            leaf_scaled, leaf_vector = pair
            kernel = build_kernel(leaf_scaled)
            return jnp.dot(leaf_vector, kernel, precision=highest)
        result = lax.map(one_leaf, (scaled_leaves, jnp.moveaxis(vector, 1, 0)))
        return jnp.moveaxis(result, 0, 1)

    def low_part(vector):
        flat = vector.reshape(num_vectors, num_points)
        total = jnp.zeros((num_vectors, num_leaves, leaf_len), jnp.float32)
        for level in range(num_levels):
            nodes = num_leaves >> level
            node_len = leaf_len << level
            right_fac = v_factors[level].reshape(num_rank, nodes, node_len)
            coef = jnp.einsum('rnp,knp->nrk', right_fac, flat.reshape(num_vectors, nodes, node_len), precision=highest)
            sibling = coef.reshape(nodes // 2, 2, num_rank, num_vectors)[:, ::-1].reshape(nodes, num_rank, num_vectors)
            left_fac = u_factors[level].reshape(num_rank, nodes, node_len)
            total = total + jnp.einsum('rnp,nrk->knp', left_fac, sibling, precision=highest).reshape(num_vectors, num_leaves, leaf_len)
        return total

    def operate(vector):
        return live_mask[None] * (dense_part(vector) + noise_var[0] * vector + low_part(vector))
    start = live_mask[None] * ordered
    beta = jnp.sqrt(lax.optimization_barrier(jnp.sum(start * start, axis=(1, 2))) + epsilon)
    basis = [start / beta[:, None, None]]
    columns = []
    for step_idx in range(ITERS):
        image = operate(basis[step_idx])
        column = [lax.optimization_barrier(jnp.sum(basis[row_idx] * image, axis=(1, 2))) for row_idx in range(step_idx + 1)]
        for row_idx in range(step_idx + 1):
            image = image - column[row_idx][:, None, None] * basis[row_idx]
        length = jnp.sqrt(lax.optimization_barrier(jnp.sum(image * image, axis=(1, 2))) + epsilon)
        column.append(length)
        columns.append(column)
        if step_idx + 1 < ITERS:
            basis.append(image / length[:, None, None])
    weights = least_squares(columns, beta)
    solved = weights[0][:, None, None] * basis[0]
    for step_idx in range(1, ITERS):
        solved = solved + weights[step_idx][:, None, None] * basis[step_idx]
    leaf_rows = jnp.arange(num_leaves, dtype=jnp.int32)[:, None]
    placed = jnp.zeros((num_vectors, num_leaves, leaf_len), jnp.float32).at[:, leaf_rows, leaf_order].set(solved)
    return placed.reshape(num_vectors, num_points)
```

```python
import functools
import math

import jax
import jax.numpy as jnp
from jax import lax
from jax.experimental import pallas as pl
from jax.experimental.pallas import tpu as pltpu
from jax.sharding import PartitionSpec as P

AXES = ("gx", "gy")
LANES = 128
TILE = 256
EPSILON = 1e-06
DISTANCE_SCALE = math.sqrt(3.0) / math.log(2.0)
LN2 = math.log(2.0)
f32 = jnp.float32
bf16 = jnp.bfloat16


def split(x, parts):
    pieces = []
    for part in range(parts):
        piece = x.astype(bf16)
        pieces.append(piece)
        if part + 1 < parts:
            x = x - piece.astype(f32)
    return pieces


def dot(a, b):
    return lax.dot_general(a, b, (((1,), (0,)), ((), ())), preferred_element_type=f32)


def dot_nt(a, b):
    return lax.dot_general(a, b, (((1,), (1,)), ((), ())), preferred_element_type=f32)


def live_row(size, length):
    return lax.broadcasted_iota(jnp.int32, (1, length), 1) < size


def levels_of(num, levels):
    me = lax.axis_index("gx") * lax.axis_size("gy") + lax.axis_index("gy")
    apart = lax.broadcasted_iota(jnp.int32, (num, 1), 0) ^ me
    level = jnp.full((num, 1), -1, jnp.int32)
    for bit in range(levels):
        level = level + (apart >= (1 << bit)).astype(jnp.int32)
    return level


def diagonal(vectors):
    shape = (LANES // vectors, LANES)
    return lax.broadcasted_iota(jnp.int32, shape, 1) // vectors == lax.broadcasted_iota(
        jnp.int32, shape, 0
    )


def slot_mask(vectors, slot):
    shape = (vectors, LANES)
    return (
        lax.broadcasted_iota(jnp.int32, shape, 1)
        == lax.broadcasted_iota(jnp.int32, shape, 0) + slot * vectors
    )


def pack_dots(pairs, vectors):
    rows = jnp.zeros((vectors, LANES), f32)
    for slot, (a, b) in enumerate(pairs):
        total = jnp.sum(a * b, axis=1, keepdims=True)
        rows = jnp.where(slot_mask(vectors, slot), total, rows)
    return jnp.sum(rows, axis=0, keepdims=True)


def unpack_dots(received, count, vectors):
    total = jnp.sum(received, axis=0, keepdims=True)
    out = []
    for slot in range(count):
        chosen = jnp.where(slot_mask(vectors, slot), total, 0.0)
        out.append(jnp.sum(chosen, axis=1, keepdims=True))
    return out


def send_coefs(vector, high, low, pay_ref, dots, levels, rank):
    vectors = vector.shape[0]
    group = LANES // vectors
    num = pay_ref.shape[0]
    first, second = split(vector, 2)
    wide = jnp.concatenate([first] * group + [second] * group, axis=0)
    both = dot_nt(high, wide) + dot_nt(low, wide)
    both = both[:, :LANES] + both[:, LANES:]
    mask = diagonal(vectors)
    level = levels_of(num, levels)
    for block in range(rank // group):
        rows = jnp.zeros((num, LANES), f32)
        for lev in range(levels):
            start = lev * rank + block * group
            piece = jnp.where(mask, both[start : start + group], 0.0)
            rows = jnp.where(level == lev, jnp.sum(piece, axis=0, keepdims=True), rows)
        pay_ref[:, block * LANES : (block + 1) * LANES] = rows
    pay_ref[:, rank * vectors :] = jnp.broadcast_to(dots, (num, LANES))


def receive_coefs(recv_ref, vectors, levels, rank):
    num = recv_ref.shape[0]
    group = LANES // vectors
    mask = diagonal(vectors)
    level = levels_of(num, levels)
    pieces = []
    for lev in range(levels):
        for block in range(rank // group):
            part = recv_ref[:, block * LANES : (block + 1) * LANES]
            total = jnp.sum(jnp.where(level == lev, part, 0.0), axis=0, keepdims=True)
            pieces.append(jnp.where(mask, jnp.broadcast_to(total, mask.shape), 0.0))
    flipped = jnp.concatenate(pieces, axis=0).T
    out = flipped[:vectors]
    for row in range(1, group):
        out = out + flipped[row * vectors : (row + 1) * vectors]
    return out


def expand(coefs, high, low):
    vectors = coefs.shape[0]
    stacked = jnp.concatenate(split(coefs, 3), axis=0)
    out = dot(stacked, high) + dot(stacked, low)
    return out[:vectors] + out[vectors : 2 * vectors] + out[2 * vectors :]


def one_hot(row, length):
    width = row.shape[1]
    steps = lax.broadcasted_iota(jnp.int32, (TILE, width), 0).astype(f32).astype(bf16)
    pieces = []
    for base in range(0, length, TILE):
        local = (row - base).astype(f32)
        local = jnp.broadcast_to(local, (TILE, width)).astype(bf16)
        pieces.append(jnp.where(steps == local, jnp.ones((), bf16), jnp.zeros((), bf16)))
    return jnp.concatenate(pieces, axis=0)


def start_body(
    sizes_ref, scales_ref, order_ref, rhs_ref, coords_ref, v_ref,
    start_ref, points_ref, pay_ref, v1_ref, v2_ref, pad_ref, *, levels, rank,
):
    vectors, length = rhs_ref.shape
    dims = coords_ref.shape[0]
    pad_ref[...] = jnp.zeros(pad_ref.shape, f32)
    pad_ref[:dims, :] = coords_ref[...]
    stacked = jnp.concatenate(
        [p.astype(f32) for p in split(rhs_ref[...], 3)]
        + [p.astype(f32) for p in split(pad_ref[...], 3)],
        axis=0,
    ).astype(bf16)
    rows = pad_ref.shape[0]
    row_id = lax.broadcasted_iota(jnp.int32, (rows, 1), 0)
    scale = jnp.zeros((rows, 1), f32)
    for dim in range(dims):
        scale = jnp.where(row_id == dim, scales_ref[dim] * DISTANCE_SCALE, scale)
    for base in range(0, length, TILE):
        chosen = dot(stacked, one_hot(order_ref[:, base : base + TILE], length))
        lane = base + lax.broadcasted_iota(jnp.int32, (1, TILE), 1)
        value = chosen[:vectors] + chosen[vectors : 2 * vectors] + chosen[2 * vectors : 3 * vectors]
        start_ref[:, base : base + TILE] = jnp.where(lane < sizes_ref[0], value, 0.0)
        rest = chosen[3 * vectors :]
        value = rest[:rows] + rest[rows : 2 * rows] + rest[2 * rows :]
        points_ref[:, base : base + TILE] = value * scale
    high, low = split(v_ref[...], 2)
    v1_ref[...] = high
    v2_ref[...] = low
    start = start_ref[...]
    dots = pack_dots([(start, start)], vectors)
    send_coefs(start, high, low, pay_ref, dots, levels, rank)


def dense(vector, high_ref, low_ref, acc_ref):
    vectors, length = vector.shape
    stacked = jnp.concatenate(split(vector, 3), axis=0)
    offset = 0
    for base in range(0, length, TILE):
        width = length - base
        own = stacked[:, base : base + TILE]
        high = high_ref[:, offset : offset + width]
        low = low_ref[:, offset : offset + width]
        part = dot(own, high) + dot(own, low)
        if base == 0:
            acc_ref[...] = part
        else:
            acc_ref[:, base:] += part
        if width > TILE:
            rest = stacked[:, base + TILE :]
            acc_ref[:, base : base + TILE] += dot_nt(rest, high[:, TILE:]) + dot_nt(
                rest, low[:, TILE:]
            )
        offset += width
    out = acc_ref[...]
    return out[:vectors] + out[vectors : 2 * vectors] + out[2 * vectors :]


def build_body(
    noise_ref, points_ref, start_ref, u_ref, high_ref, low_ref, image_ref, u1_ref, u2_ref,
    column_ref, acc_ref, *, dims,
):
    length = points_ref.shape[1]
    step = 16
    column_ref[...] = points_ref[...].T
    high, low = split(u_ref[...], 2)
    u1_ref[...] = high
    u2_ref[...] = low
    offset = 0
    for base in range(0, length, TILE):
        width = length - base

        def rows_step(index, carry, base=base, width=width, offset=offset):
            row = pl.multiple_of(index * step, step)
            square = None
            for dim in range(dims):
                differ = (
                    column_ref[pl.ds(base + row, step), dim : dim + 1]
                    - points_ref[dim : dim + 1, base:]
                )
                square = differ * differ if square is None else square + differ * differ
            square = jnp.maximum(square, 1e-30)
            distance = square * lax.rsqrt(square)
            value = (1.0 + LN2 * distance) * jnp.exp2(-distance)
            high, low = split(value, 2)
            high_ref[pl.ds(row, step), offset : offset + width] = high
            low_ref[pl.ds(row, step), offset : offset + width] = low
            return carry

        lax.fori_loop(0, TILE // step, rows_step, 0)
        offset += width
    start = start_ref[...]
    image_ref[...] = dense(start, high_ref, low_ref, acc_ref) + noise_ref[0] * start


def dense_body(noise_ref, vector_ref, high_ref, low_ref, image_ref, acc_ref):
    vector = vector_ref[...]
    image_ref[...] = dense(vector, high_ref, low_ref, acc_ref) + noise_ref[0] * vector


def inverse_body(order_ref, inverse_ref):
    length = order_ref.shape[1]
    place = lax.broadcasted_iota(jnp.int32, (8, TILE), 1).astype(f32)
    row_id = lax.broadcasted_iota(jnp.int32, (8, TILE), 0)
    total = jnp.zeros((8, length), f32)
    for base in range(0, length, TILE):
        weights = jnp.where(row_id == 0, place, float(base // TILE))
        hot = one_hot(order_ref[:, base : base + TILE], length)
        total = total + dot_nt(weights.astype(bf16), hot)
    inverse_ref[...] = (total[0:1] + total[1:2] * float(TILE)).astype(jnp.int32)


def first_body(
    sizes_ref, recv_ref, image_ref, start_ref, u1_ref, u2_ref, v1_ref, v2_ref,
    q0_ref, w0_ref, scal_ref, pay_ref, *, levels, rank,
):
    vectors, length = start_ref.shape
    live = live_row(sizes_ref[0], length)
    (norm,) = unpack_dots(recv_ref[:, rank * vectors :], 1, vectors)
    beta = jnp.sqrt(norm + EPSILON)
    inverse = 1.0 / beta
    distant = expand(receive_coefs(recv_ref, vectors, levels, rank), u1_ref[...], u2_ref[...])
    w0 = jnp.where(live, image_ref[...] + distant, 0.0) * inverse
    q0 = start_ref[...] * inverse
    q0_ref[...] = q0
    w0_ref[...] = w0
    scal_ref[...] = jnp.broadcast_to(beta, scal_ref.shape)
    dots = pack_dots([(q0, q0), (q0, w0), (w0, w0)], vectors)
    send_coefs(w0, v1_ref[...], v2_ref[...], pay_ref, dots, levels, rank)


def put_scalars(scal_ref, values):
    lane = lax.broadcasted_iota(jnp.int32, scal_ref.shape, 1)
    out = jnp.zeros(scal_ref.shape, f32)
    for slot, value in enumerate(values):
        out = jnp.where(lane == slot, value, out)
    scal_ref[...] = out


def get_scalars(scal_ref, count):
    return [scal_ref[:, slot : slot + 1] for slot in range(count)]


def second_body(
    sizes_ref, recv_ref, image_ref, q0_ref, w0_ref, old_ref, u1_ref, u2_ref, v1_ref, v2_ref,
    q1_ref, w1_ref, scal_ref, pay_ref, *, levels, rank,
):
    vectors, length = q0_ref.shape
    live = live_row(sizes_ref[0], length)
    (beta,) = get_scalars(old_ref, 1)
    g00, h00, norm = unpack_dots(recv_ref[:, rank * vectors :], 3, vectors)
    rest = norm - 2.0 * h00 * h00 + h00 * h00 * g00
    h10 = jnp.sqrt(jnp.maximum(rest, 0.0) + EPSILON)
    inverse = 1.0 / h10
    put_scalars(scal_ref, [beta, g00, h00, h10])
    distant = expand(receive_coefs(recv_ref, vectors, levels, rank), u1_ref[...], u2_ref[...])
    w0 = w0_ref[...]
    q0 = q0_ref[...]
    q1 = (w0 - h00 * q0) * inverse
    w1 = (jnp.where(live, image_ref[...] + distant, 0.0) - h00 * w0) * inverse
    q1_ref[...] = q1
    w1_ref[...] = w1
    dots = pack_dots([(q0, w1), (q1, w1), (w1, w1), (q0, q1), (q1, q1)], vectors)
    send_coefs(w1, v1_ref[...], v2_ref[...], pay_ref, dots, levels, rank)


def third_body(
    sizes_ref, recv_ref, image_ref, q0_ref, q1_ref, w0_ref, w1_ref, old_ref, u1_ref, u2_ref,
    q2_ref, scal_ref, pay_ref, *, levels, rank,
):
    vectors, length = q0_ref.shape
    live = live_row(sizes_ref[0], length)
    beta, g00, h00, h10 = get_scalars(old_ref, 4)
    h01, h11, norm, g01, g11 = unpack_dots(recv_ref[:, rank * vectors :], 5, vectors)
    rest = (
        norm - 2.0 * (h01 * h01 + h11 * h11)
        + (h01 * h01 * g00 + h11 * h11 * g11 + 2.0 * h01 * h11 * g01)
    )
    h21 = jnp.sqrt(jnp.maximum(rest, 0.0) + EPSILON)
    inverse = 1.0 / h21
    put_scalars(scal_ref, [beta, g00, h00, h10, g01, g11, h01, h11, h21])
    distant = expand(receive_coefs(recv_ref, vectors, levels, rank), u1_ref[...], u2_ref[...])
    w0 = w0_ref[...]
    w1 = w1_ref[...]
    q0 = q0_ref[...]
    q1 = q1_ref[...]
    q2 = (w1 - h01 * q0 - h11 * q1) * inverse
    image = jnp.where(live, image_ref[...] + distant, 0.0)
    w2 = (image - h01 * w0 - h11 * w1) * inverse
    q2_ref[...] = q2
    dots = pack_dots(
        [(q0, w2), (q1, w2), (q2, w2), (w2, w2), (q0, q2), (q1, q2), (q2, q2)], vectors
    )
    pay_ref[...] = jnp.broadcast_to(dots, pay_ref.shape)


def least_squares(columns, beta):
    count_cols = len(columns)
    cosines = []
    sines = []
    target = [beta] + [jnp.zeros_like(beta)] * count_cols
    upper = []
    for column_idx in range(count_cols):
        entries = list(columns[column_idx])
        for row_idx in range(column_idx):
            first_val = entries[row_idx]
            second_val = entries[row_idx + 1]
            entries[row_idx] = cosines[row_idx] * first_val + sines[row_idx] * second_val
            entries[row_idx + 1] = -sines[row_idx] * first_val + cosines[row_idx] * second_val
        first_val = entries[column_idx]
        second_val = entries[column_idx + 1]
        radius = jnp.sqrt(first_val * first_val + second_val * second_val)
        cosines.append(first_val / radius)
        sines.append(second_val / radius)
        entries[column_idx] = radius
        carried = target[column_idx]
        target[column_idx] = cosines[column_idx] * carried
        target[column_idx + 1] = -sines[column_idx] * carried
        upper.append(entries[: column_idx + 1])
    weights = [None] * count_cols
    for column_idx in reversed(range(count_cols)):
        accum = target[column_idx]
        for later_idx in range(column_idx + 1, count_cols):
            accum = accum - upper[later_idx][column_idx] * weights[later_idx]
        weights[column_idx] = accum / upper[column_idx][column_idx]
    return weights


def last_body(recv_ref, q0_ref, q1_ref, q2_ref, old_ref, inverse_ref, out_ref):
    vectors, length = q0_ref.shape
    beta, g00, h00, h10, g01, g11, h01, h11, h21 = get_scalars(old_ref, 9)
    h02, h12, h22, norm, g02, g12, g22 = unpack_dots(recv_ref[...], 7, vectors)
    rest = (
        norm - 2.0 * (h02 * h02 + h12 * h12 + h22 * h22)
        + (h02 * h02 * g00 + h12 * h12 * g11 + h22 * h22 * g22)
        + 2.0 * (h02 * h12 * g01 + h02 * h22 * g02 + h12 * h22 * g12)
    )
    h32 = jnp.sqrt(jnp.maximum(rest, 0.0) + EPSILON)
    y0, y1, y2 = least_squares([[h00, h10], [h01, h11, h21], [h02, h12, h22, h32]], beta)
    solved = y0 * q0_ref[...] + y1 * q1_ref[...] + y2 * q2_ref[...]
    stacked = jnp.concatenate(split(solved, 3), axis=0)
    for base in range(0, length, TILE):
        placed = dot(stacked, one_hot(inverse_ref[:, base : base + TILE], length))
        out_ref[:, base : base + TILE] = (
            placed[:vectors] + placed[vectors : 2 * vectors] + placed[2 * vectors :]
        )


def call(body, outs, args, smem=0, scratch=(), flops=0, limit=20, name=None):
    smem_spec = pl.BlockSpec(memory_space=pltpu.SMEM)
    vmem_spec = pl.BlockSpec(memory_space=pltpu.VMEM)
    specs = [smem_spec] * smem + [vmem_spec] * (len(args) - smem)
    total = sum(math.prod(a.shape) * a.dtype.itemsize for a in list(args) + list(outs))
    return pl.pallas_call(
        body,
        out_shape=list(outs),
        in_specs=specs,
        out_specs=[vmem_spec] * len(outs),
        scratch_shapes=list(scratch),
        compiler_params=pltpu.CompilerParams(vmem_limit_bytes=limit * 1024 * 1024),
        cost_estimate=pl.CostEstimate(flops=flops, bytes_accessed=total, transcendentals=0),
        name=name,
    )(*args)


def exchange(payload):
    return lax.all_to_all(payload, AXES, 0, 0, tiled=True)


def per_device(
    coordinates, rhs, leaf_order, leaf_sizes, inverse_scales, noise_var, u_factors, v_factors
):
    vectors, length = rhs.shape
    dims = coordinates.shape[0]
    levels, rank, _ = u_factors.shape
    num = lax.axis_size("gx") * lax.axis_size("gy")
    blocks = length // TILE
    packed = TILE * (blocks * (blocks + 1) // 2)
    padded = -(-dims // 8) * 8
    u_flat = u_factors.reshape(levels * rank, length)
    v_flat = v_factors.reshape(levels * rank, length)

    def shaped(*shape, dtype=f32):
        return jax.ShapeDtypeStruct(shape, dtype)

    field = shaped(vectors, length)
    factor = shaped(levels * rank, length, dtype=bf16)
    scalars = shaped(vectors, LANES)
    message = shaped(num, rank * vectors + LANES)
    acc = pltpu.VMEM((3 * vectors, length), f32)
    sizes = dict(levels=levels, rank=rank)
    small = 2 * levels * rank * length * 256

    start, points, pay, v1, v2 = call(
        functools.partial(start_body, **sizes),
        [field, shaped(padded, length), message, factor, factor],
        [leaf_sizes, inverse_scales, leaf_order, rhs, coordinates, v_flat],
        smem=2, scratch=[pltpu.VMEM((padded, length), f32)], flops=small, name="start",
    )
    recv = exchange(pay)
    k1, k2, image, u1, u2 = call(
        functools.partial(build_body, dims=dims),
        [shaped(TILE, packed, dtype=bf16)] * 2 + [field, factor, factor],
        [noise_var, points, start, u_flat],
        smem=1, scratch=[pltpu.VMEM((length, padded), f32), acc],
        flops=2 * length * length * 256, limit=30, name="build",
    )
    (inverse,) = call(
        inverse_body, [shaped(1, length, dtype=jnp.int32)], [leaf_order],
        flops=2 * length * length * 64, name="inverse",
    )

    def near(vector, name):
        (out,) = call(
            dense_body, [field], [noise_var, vector, k1, k2],
            smem=1, scratch=[acc], flops=2 * length * length * 128, name=name,
        )
        return out

    q0, w0, scal, pay = call(
        functools.partial(first_body, **sizes),
        [field, field, scalars, message],
        [leaf_sizes, recv, image, start, u1, u2, v1, v2],
        smem=1, flops=small, name="first",
    )
    recv = exchange(pay)
    image = near(w0, "near1")
    q1, w1, scal, pay = call(
        functools.partial(second_body, **sizes),
        [field, field, scalars, message],
        [leaf_sizes, recv, image, q0, w0, scal, u1, u2, v1, v2],
        smem=1, flops=small, name="second",
    )
    recv = exchange(pay)
    image = near(w1, "near2")
    q2, scal, pay = call(
        functools.partial(third_body, **sizes),
        [field, scalars, shaped(num, LANES)],
        [leaf_sizes, recv, image, q0, q1, w0, w1, scal, u1, u2],
        smem=1, flops=small, name="third",
    )
    recv = exchange(pay)
    (out,) = call(
        last_body, [field], [recv, q0, q1, q2, scal, inverse], flops=small, name="last"
    )
    return out


def solution(mesh):
    in_specs = (
        P(None, AXES),
        P(None, AXES),
        P(AXES, None),
        P(AXES),
        P(),
        P(),
        P(None, None, AXES),
        P(None, None, AXES),
    )
    return jax.shard_map(
        per_device, mesh=mesh, in_specs=in_specs, out_specs=P(None, AXES), check_vma=False
    )
```

```python
import functools
import math

import jax
import jax.numpy as jnp
from jax import lax
from jax.experimental import pallas as pl
from jax.experimental.pallas import tpu as pltpu
from jax.sharding import PartitionSpec as P

AXES = ("gx", "gy")
LANES = 128
TILE = 256
EPSILON = 1e-06
DISTANCE_SCALE = math.sqrt(3.0) / math.log(2.0)
LN2 = math.log(2.0)
f32 = jnp.float32
bf16 = jnp.bfloat16


def split(x, parts):
    pieces = []
    for part in range(parts):
        piece = x.astype(bf16)
        pieces.append(piece)
        if part + 1 < parts:
            x = x - piece.astype(f32)
    return pieces


def dot(a, b):
    return lax.dot_general(a, b, (((1,), (0,)), ((), ())), preferred_element_type=f32)


def dot_nt(a, b):
    return lax.dot_general(a, b, (((1,), (1,)), ((), ())), preferred_element_type=f32)


def live_row(size, length):
    return lax.broadcasted_iota(jnp.int32, (1, length), 1) < size


def levels_of(num, levels):
    me = lax.axis_index("gx") * lax.axis_size("gy") + lax.axis_index("gy")
    apart = lax.broadcasted_iota(jnp.int32, (num, 1), 0) ^ me
    level = jnp.full((num, 1), -1, jnp.int32)
    for bit in range(levels):
        level = level + (apart >= (1 << bit)).astype(jnp.int32)
    return level


def diagonal(vectors):
    shape = (LANES // vectors, LANES)
    return lax.broadcasted_iota(jnp.int32, shape, 1) // vectors == lax.broadcasted_iota(
        jnp.int32, shape, 0
    )


def slot_mask(vectors, slot):
    shape = (vectors, LANES)
    return (
        lax.broadcasted_iota(jnp.int32, shape, 1)
        == lax.broadcasted_iota(jnp.int32, shape, 0) + slot * vectors
    )


def pack_dots(pairs, vectors):
    rows = jnp.zeros((vectors, LANES), f32)
    for slot, (a, b) in enumerate(pairs):
        total = jnp.sum(a * b, axis=1, keepdims=True)
        rows = jnp.where(slot_mask(vectors, slot), total, rows)
    return jnp.sum(rows, axis=0, keepdims=True)


def unpack_dots(received, count, vectors):
    total = jnp.sum(received, axis=0, keepdims=True)
    out = []
    for slot in range(count):
        chosen = jnp.where(slot_mask(vectors, slot), total, 0.0)
        out.append(jnp.sum(chosen, axis=1, keepdims=True))
    return out


def send_coefs(vector, high, low, pay_ref, dots, levels, rank):
    vectors = vector.shape[0]
    group = LANES // vectors
    num = pay_ref.shape[0]
    first, second = split(vector, 2)
    wide = jnp.concatenate([first] * group + [second] * group, axis=0)
    both = dot_nt(high, wide) + dot_nt(low, wide)
    both = both[:, :LANES] + both[:, LANES:]
    mask = diagonal(vectors)
    level = levels_of(num, levels)
    for block in range(rank // group):
        rows = jnp.zeros((num, LANES), f32)
        for lev in range(levels):
            start = lev * rank + block * group
            piece = jnp.where(mask, both[start : start + group], 0.0)
            rows = jnp.where(level == lev, jnp.sum(piece, axis=0, keepdims=True), rows)
        pay_ref[:, 0, block * LANES : (block + 1) * LANES] = rows
    pay_ref[:, 0, rank * vectors :] = jnp.broadcast_to(dots, (num, LANES))


def receive_coefs(recv_ref, vectors, levels, rank):
    num = recv_ref.shape[0]
    group = LANES // vectors
    mask = diagonal(vectors)
    level = levels_of(num, levels)
    pieces = []
    for lev in range(levels):
        for block in range(rank // group):
            part = recv_ref[:, 0, block * LANES : (block + 1) * LANES]
            total = jnp.sum(jnp.where(level == lev, part, 0.0), axis=0, keepdims=True)
            pieces.append(jnp.where(mask, jnp.broadcast_to(total, mask.shape), 0.0))
    flipped = jnp.concatenate(pieces, axis=0).T
    out = flipped[:vectors]
    for row in range(1, group):
        out = out + flipped[row * vectors : (row + 1) * vectors]
    return out


def expand(coefs, high, low):
    vectors = coefs.shape[0]
    stacked = jnp.concatenate(split(coefs, 3), axis=0)
    out = dot(stacked, high) + dot(stacked, low)
    return out[:vectors] + out[vectors : 2 * vectors] + out[2 * vectors :]


def one_hot(row, length):
    width = row.shape[1]
    steps = lax.broadcasted_iota(jnp.int32, (TILE, width), 0).astype(f32).astype(bf16)
    pieces = []
    for base in range(0, length, TILE):
        local = (row - base).astype(f32)
        local = jnp.broadcast_to(local, (TILE, width)).astype(bf16)
        pieces.append(jnp.where(steps == local, jnp.ones((), bf16), jnp.zeros((), bf16)))
    return jnp.concatenate(pieces, axis=0)


def start_body(
    sizes_ref, scales_ref, order_hbm, rhs_hbm, coords_hbm, v_hbm,
    start_ref, points_ref, pay_ref, v1_hbm, v2_hbm,
    order_ref, rhs_ref, coords_ref, pad_ref, v_ref, v1_ref, v2_ref, sem, *, levels, rank,
):
    loads = [
        pltpu.make_async_copy(source, target, sem.at[n])
        for n, (source, target) in enumerate(
            [(order_hbm, order_ref), (rhs_hbm, rhs_ref), (coords_hbm, coords_ref), (v_hbm, v_ref)]
        )
    ]
    for load in loads:
        load.start()
    vectors, length = rhs_ref.shape
    dims = coords_ref.shape[0]
    pad_ref[...] = jnp.zeros(pad_ref.shape, f32)
    for load in loads[:3]:
        load.wait()
    pad_ref[:dims, :] = coords_ref[...]
    stacked = jnp.concatenate(
        [p.astype(f32) for p in split(rhs_ref[...], 3)]
        + [p.astype(f32) for p in split(pad_ref[...], 3)],
        axis=0,
    ).astype(bf16)
    rows = pad_ref.shape[0]
    row_id = lax.broadcasted_iota(jnp.int32, (rows, 1), 0)
    scale = jnp.zeros((rows, 1), f32)
    for dim in range(dims):
        scale = jnp.where(row_id == dim, scales_ref[dim] * DISTANCE_SCALE, scale)
    for base in range(0, length, TILE):
        chosen = dot(stacked, one_hot(order_ref[:, base : base + TILE], length))
        lane = base + lax.broadcasted_iota(jnp.int32, (1, TILE), 1)
        value = chosen[:vectors] + chosen[vectors : 2 * vectors] + chosen[2 * vectors : 3 * vectors]
        start_ref[:, base : base + TILE] = jnp.where(lane < sizes_ref[0], value, 0.0)
        rest = chosen[3 * vectors :]
        value = rest[:rows] + rest[rows : 2 * rows] + rest[2 * rows :]
        points_ref[:, base : base + TILE] = value * scale
    loads[3].wait()
    high, low = split(v_ref[...], 2)
    v1_ref[...] = high
    v2_ref[...] = low
    stores = [
        pltpu.make_async_copy(v1_ref, v1_hbm, sem.at[4]),
        pltpu.make_async_copy(v2_ref, v2_hbm, sem.at[5]),
    ]
    for store in stores:
        store.start()
    start = start_ref[...]
    dots = pack_dots([(start, start)], vectors)
    send_coefs(start, high, low, pay_ref, dots, levels, rank)
    for store in stores:
        store.wait()


def add_panel(stacked, high_ref, low_ref, acc_ref, base, offset):
    width = acc_ref.shape[1] - base
    own = stacked[:, base : base + TILE]
    for half in (high_ref, low_ref):
        acc_ref[:, base:] += dot(own, half[:, offset : offset + width])
        if width > TILE:
            acc_ref[:, base : base + TILE] += dot_nt(
                stacked[:, base + TILE :], half[:, offset + TILE : offset + width]
            )


def finish(acc_ref, noise_ref, vector):
    vectors = vector.shape[0]
    out = acc_ref[...]
    out = out[:vectors] + out[vectors : 2 * vectors] + out[2 * vectors :]
    return LN2 * out + noise_ref[0] * vector


def panels(length):
    offset = 0
    for base in range(0, length, TILE):
        yield base, offset, length - base
        offset += length - base


def build_body(
    noise_ref, points_ref, start_ref, u_hbm, high_hbm, low_hbm, image_ref, u1_ref, u2_ref,
    u_ref, wide_ref, high_ref, low_ref, acc_ref, sem, *, dims,
):
    length = points_ref.shape[1]
    step = 16
    load = pltpu.make_async_copy(u_hbm, u_ref, sem.at[0])
    load.start()
    columns = points_ref[...].T
    for dim in range(dims):
        wide_ref[dim] = jnp.broadcast_to(columns[:, dim : dim + 1], (length, LANES))
    start = start_ref[...]
    stacked = jnp.concatenate(split(start, 3), axis=0)
    acc_ref[...] = jnp.zeros(acc_ref.shape, f32)
    copies = []
    for base, offset, width in panels(length):
        for row in range(0, TILE, step):
            column = [wide_ref[dim, base + row : base + row + step, :] for dim in range(dims)]
            for lane in range(base, length, LANES):
                square = None
                for dim in range(dims):
                    differ = column[dim] - points_ref[dim : dim + 1, lane : lane + LANES]
                    square = differ * differ if square is None else square + differ * differ
                square = jnp.maximum(square, 1e-30)
                distance = square * lax.rsqrt(square)
                value = (1.0 / LN2 + distance) * jnp.exp2(-distance)
                high, low = split(value, 2)
                place = offset + lane - base
                high_ref[row : row + step, place : place + LANES] = high
                low_ref[row : row + step, place : place + LANES] = low
        for source, target in ((high_ref, high_hbm), (low_ref, low_hbm)):
            copy = pltpu.make_async_copy(
                source.at[:, offset : offset + width],
                target.at[:, offset : offset + width],
                sem.at[1 + len(copies)],
            )
            copy.start()
            copies.append(copy)
        add_panel(stacked, high_ref, low_ref, acc_ref, base, offset)
    image_ref[...] = finish(acc_ref, noise_ref, start)
    load.wait()
    high, low = split(u_ref[...], 2)
    u1_ref[...] = high
    u2_ref[...] = low
    for copy in copies:
        copy.wait()


def near_body(
    noise_ref, vector_ref, high_hbm, low_hbm, *refs, order
):
    if order:
        order_ref, image_ref, inverse_ref, high_ref, low_ref, acc_ref, sem = refs
    else:
        image_ref, high_ref, low_ref, acc_ref, sem = refs
    vector = vector_ref[...]
    length = vector.shape[1]
    copies = []
    for base, offset, width in panels(length):
        for source, target in ((high_hbm, high_ref), (low_hbm, low_ref)):
            copy = pltpu.make_async_copy(
                source.at[:, offset : offset + width],
                target.at[:, offset : offset + width],
                sem.at[len(copies)],
            )
            copy.start()
            copies.append(copy)
    stacked = jnp.concatenate(split(vector, 3), axis=0)
    acc_ref[...] = jnp.zeros(acc_ref.shape, f32)
    if order:
        inverse_ref[...] = inverse_of(order_ref)
    for number, (base, offset, width) in enumerate(panels(length)):
        copies[2 * number].wait()
        copies[2 * number + 1].wait()
        add_panel(stacked, high_ref, low_ref, acc_ref, base, offset)
    image_ref[...] = finish(acc_ref, noise_ref, vector)


def inverse_of(order_ref):
    length = order_ref.shape[1]
    place = lax.broadcasted_iota(jnp.int32, (8, TILE), 1).astype(f32)
    row_id = lax.broadcasted_iota(jnp.int32, (8, TILE), 0)
    total = jnp.zeros((8, length), f32)
    for base in range(0, length, TILE):
        weights = jnp.where(row_id == 0, place, float(base // TILE))
        hot = one_hot(order_ref[:, base : base + TILE], length)
        total = total + dot_nt(weights.astype(bf16), hot)
    return (total[0:1] + total[1:2] * float(TILE)).astype(jnp.int32)


def load_pair(high_hbm, low_hbm, high_ref, low_ref, sem):
    loads = [
        pltpu.make_async_copy(high_hbm, high_ref, sem.at[0]),
        pltpu.make_async_copy(low_hbm, low_ref, sem.at[1]),
    ]
    for load in loads:
        load.start()
    return loads


def first_body(
    sizes_ref, recv_ref, image_ref, start_ref, u1_ref, u2_ref, v1_hbm, v2_hbm,
    q0_ref, w0_ref, scal_ref, pay_ref, v1_ref, v2_ref, sem, *, levels, rank,
):
    loads = load_pair(v1_hbm, v2_hbm, v1_ref, v2_ref, sem)
    vectors, length = start_ref.shape
    live = live_row(sizes_ref[0], length)
    (norm,) = unpack_dots(recv_ref[:, 0, rank * vectors :], 1, vectors)
    beta = jnp.sqrt(norm + EPSILON)
    inverse = 1.0 / beta
    distant = expand(receive_coefs(recv_ref, vectors, levels, rank), u1_ref[...], u2_ref[...])
    w0 = jnp.where(live, image_ref[...] + distant, 0.0) * inverse
    q0 = start_ref[...] * inverse
    q0_ref[...] = q0
    w0_ref[...] = w0
    scal_ref[...] = jnp.broadcast_to(beta, scal_ref.shape)
    dots = pack_dots([(q0, q0), (q0, w0), (w0, w0)], vectors)
    for load in loads:
        load.wait()
    send_coefs(w0, v1_ref[...], v2_ref[...], pay_ref, dots, levels, rank)


def put_scalars(scal_ref, values):
    lane = lax.broadcasted_iota(jnp.int32, scal_ref.shape, 1)
    out = jnp.zeros(scal_ref.shape, f32)
    for slot, value in enumerate(values):
        out = jnp.where(lane == slot, value, out)
    scal_ref[...] = out


def get_scalars(scal_ref, count):
    return [scal_ref[:, slot : slot + 1] for slot in range(count)]


def second_body(
    sizes_ref, recv_ref, image_ref, q0_ref, w0_ref, old_ref, u1_ref, u2_ref, v1_hbm, v2_hbm,
    q1_ref, w1_ref, scal_ref, pay_ref, v1_ref, v2_ref, sem, *, levels, rank,
):
    loads = load_pair(v1_hbm, v2_hbm, v1_ref, v2_ref, sem)
    vectors, length = q0_ref.shape
    live = live_row(sizes_ref[0], length)
    (beta,) = get_scalars(old_ref, 1)
    g00, h00, norm = unpack_dots(recv_ref[:, 0, rank * vectors :], 3, vectors)
    rest = norm - 2.0 * h00 * h00 + h00 * h00 * g00
    h10 = jnp.sqrt(jnp.maximum(rest, 0.0) + EPSILON)
    inverse = 1.0 / h10
    put_scalars(scal_ref, [beta, g00, h00, h10])
    distant = expand(receive_coefs(recv_ref, vectors, levels, rank), u1_ref[...], u2_ref[...])
    w0 = w0_ref[...]
    q0 = q0_ref[...]
    q1 = (w0 - h00 * q0) * inverse
    w1 = (jnp.where(live, image_ref[...] + distant, 0.0) - h00 * w0) * inverse
    q1_ref[...] = q1
    w1_ref[...] = w1
    dots = pack_dots([(q0, w1), (q1, w1), (w1, w1), (q0, q1), (q1, q1)], vectors)
    for load in loads:
        load.wait()
    send_coefs(w1, v1_ref[...], v2_ref[...], pay_ref, dots, levels, rank)


def third_body(
    sizes_ref, recv_ref, image_ref, q0_ref, q1_ref, w0_ref, w1_ref, old_ref, u1_ref, u2_ref,
    q2_ref, scal_ref, pay_ref, *, levels, rank,
):
    vectors, length = q0_ref.shape
    live = live_row(sizes_ref[0], length)
    beta, g00, h00, h10 = get_scalars(old_ref, 4)
    h01, h11, norm, g01, g11 = unpack_dots(recv_ref[:, 0, rank * vectors :], 5, vectors)
    rest = (
        norm - 2.0 * (h01 * h01 + h11 * h11)
        + (h01 * h01 * g00 + h11 * h11 * g11 + 2.0 * h01 * h11 * g01)
    )
    h21 = jnp.sqrt(jnp.maximum(rest, 0.0) + EPSILON)
    inverse = 1.0 / h21
    put_scalars(scal_ref, [beta, g00, h00, h10, g01, g11, h01, h11, h21])
    distant = expand(receive_coefs(recv_ref, vectors, levels, rank), u1_ref[...], u2_ref[...])
    w0 = w0_ref[...]
    w1 = w1_ref[...]
    q0 = q0_ref[...]
    q1 = q1_ref[...]
    q2 = (w1 - h01 * q0 - h11 * q1) * inverse
    image = jnp.where(live, image_ref[...] + distant, 0.0)
    w2 = (image - h01 * w0 - h11 * w1) * inverse
    q2_ref[...] = q2
    dots = pack_dots(
        [(q0, w2), (q1, w2), (q2, w2), (w2, w2), (q0, q2), (q1, q2), (q2, q2)], vectors
    )
    num, _, width = pay_ref.shape
    pay_ref[:, 0, :] = jnp.broadcast_to(dots, (num, width))


def least_squares(columns, beta):
    count_cols = len(columns)
    cosines = []
    sines = []
    target = [beta] + [jnp.zeros_like(beta)] * count_cols
    upper = []
    for column_idx in range(count_cols):
        entries = list(columns[column_idx])
        for row_idx in range(column_idx):
            first_val = entries[row_idx]
            second_val = entries[row_idx + 1]
            entries[row_idx] = cosines[row_idx] * first_val + sines[row_idx] * second_val
            entries[row_idx + 1] = -sines[row_idx] * first_val + cosines[row_idx] * second_val
        first_val = entries[column_idx]
        second_val = entries[column_idx + 1]
        radius = jnp.sqrt(first_val * first_val + second_val * second_val)
        cosines.append(first_val / radius)
        sines.append(second_val / radius)
        entries[column_idx] = radius
        carried = target[column_idx]
        target[column_idx] = cosines[column_idx] * carried
        target[column_idx + 1] = -sines[column_idx] * carried
        upper.append(entries[: column_idx + 1])
    weights = [None] * count_cols
    for column_idx in reversed(range(count_cols)):
        accum = target[column_idx]
        for later_idx in range(column_idx + 1, count_cols):
            accum = accum - upper[later_idx][column_idx] * weights[later_idx]
        weights[column_idx] = accum / upper[column_idx][column_idx]
    return weights


def last_body(recv_ref, q0_ref, q1_ref, q2_ref, old_ref, inverse_ref, out_ref):
    vectors, length = q0_ref.shape
    beta, g00, h00, h10, g01, g11, h01, h11, h21 = get_scalars(old_ref, 9)
    h02, h12, h22, norm, g02, g12, g22 = unpack_dots(recv_ref[:, 0, :], 7, vectors)
    rest = (
        norm - 2.0 * (h02 * h02 + h12 * h12 + h22 * h22)
        + (h02 * h02 * g00 + h12 * h12 * g11 + h22 * h22 * g22)
        + 2.0 * (h02 * h12 * g01 + h02 * h22 * g02 + h12 * h22 * g12)
    )
    h32 = jnp.sqrt(jnp.maximum(rest, 0.0) + EPSILON)
    y0, y1, y2 = least_squares([[h00, h10], [h01, h11, h21], [h02, h12, h22, h32]], beta)
    solved = y0 * q0_ref[...] + y1 * q1_ref[...] + y2 * q2_ref[...]
    stacked = jnp.concatenate(split(solved, 3), axis=0)
    for base in range(0, length, TILE):
        placed = dot(stacked, one_hot(inverse_ref[:, base : base + TILE], length))
        out_ref[:, base : base + TILE] = (
            placed[:vectors] + placed[vectors : 2 * vectors] + placed[2 * vectors :]
        )


def call(body, outs, args, scratch=(), flops=0, limit=20000, name=None):
    spaces = dict(s=pltpu.SMEM, v=pltpu.VMEM, h=pltpu.HBM)
    total = sum(math.prod(a.shape) * a.dtype.itemsize for _, a in list(args) + list(outs))
    return pl.pallas_call(
        body,
        out_shape=[pltpu.HBM(a.shape, a.dtype) if m == "h" else a for m, a in outs],
        in_specs=[pl.BlockSpec(memory_space=spaces[m]) for m, _ in args],
        out_specs=[pl.BlockSpec(memory_space=spaces[m]) for m, _ in outs],
        scratch_shapes=list(scratch),
        compiler_params=pltpu.CompilerParams(vmem_limit_bytes=limit * 1024),
        cost_estimate=pl.CostEstimate(flops=flops, bytes_accessed=total, transcendentals=0),
        name=name,
    )(*[pltpu.with_memory_space_constraint(a, pltpu.HBM) if m == "h" else a for m, a in args])


def exchange(payload):
    return lax.all_to_all(payload, AXES, 0, 0, tiled=True)


def per_device(
    coordinates, rhs, leaf_order, leaf_sizes, inverse_scales, noise_var, u_factors, v_factors
):
    vectors, length = rhs.shape
    dims = coordinates.shape[0]
    levels, rank, _ = u_factors.shape
    num = lax.axis_size("gx") * lax.axis_size("gy")
    blocks = length // TILE
    packed = TILE * (blocks * (blocks + 1) // 2)
    padded = -(-dims // 8) * 8
    u_flat = u_factors.reshape(levels * rank, length)
    v_flat = v_factors.reshape(levels * rank, length)

    def shaped(*shape, dtype=f32):
        return jax.ShapeDtypeStruct(shape, dtype)

    field = ("v", shaped(vectors, length))
    factor = shaped(levels * rank, length, dtype=bf16)
    scalars = ("v", shaped(vectors, LANES))
    message = ("v", shaped(num, 1, rank * vectors + LANES))
    panel = shaped(TILE, packed, dtype=bf16)
    acc = pltpu.VMEM((3 * vectors, length), f32)
    panel_space = pltpu.VMEM((TILE, packed), bf16)
    factor_space = pltpu.VMEM((levels * rank, length), bf16)
    whole_space = pltpu.VMEM((levels * rank, length), f32)
    sizes = dict(levels=levels, rank=rank)
    small = 2 * levels * rank * length * 256

    def arrays(memory, *values):
        return [(memory, value) for value in values]

    start, points, pay, v1, v2 = call(
        functools.partial(start_body, **sizes),
        [field, ("v", shaped(padded, length)), message, ("h", factor), ("h", factor)],
        arrays("s", leaf_sizes, inverse_scales)
        + arrays("h", leaf_order, rhs, coordinates, v_flat),
        scratch=[
            pltpu.VMEM((1, length), jnp.int32),
            pltpu.VMEM((vectors, length), f32),
            pltpu.VMEM((dims, length), f32),
            pltpu.VMEM((padded, length), f32),
            whole_space,
            factor_space,
            factor_space,
            pltpu.SemaphoreType.DMA((6,)),
        ],
        flops=small, name="start",
    )
    recv = exchange(pay)
    k1, k2, image, u1, u2 = call(
        functools.partial(build_body, dims=dims),
        [("h", panel), ("h", panel), field, ("v", factor), ("v", factor)],
        arrays("s", noise_var) + arrays("v", points, start) + arrays("h", u_flat),
        scratch=[
            whole_space,
            pltpu.VMEM((dims, length, LANES), f32),
            panel_space,
            panel_space,
            acc,
            pltpu.SemaphoreType.DMA((1 + 2 * blocks,)),
        ],
        flops=2 * length * length * 256, limit=40000, name="build",
    )

    def near(vector, name, order):
        return call(
            functools.partial(near_body, order=order),
            [field] + ([("v", shaped(1, length, dtype=jnp.int32))] if order else []),
            arrays("s", noise_var) + arrays("v", vector) + arrays("h", k1, k2)
            + (arrays("v", leaf_order) if order else []),
            scratch=[panel_space, panel_space, acc, pltpu.SemaphoreType.DMA((2 * blocks,))],
            flops=2 * length * length * 128, limit=30000, name=name,
        )

    pair_space = [factor_space, factor_space, pltpu.SemaphoreType.DMA((2,))]
    q0, w0, scal, pay = call(
        functools.partial(first_body, **sizes),
        [field, field, scalars, message],
        arrays("s", leaf_sizes) + arrays("v", recv, image, start, u1, u2) + arrays("h", v1, v2),
        scratch=pair_space, flops=small, name="first",
    )
    recv = exchange(pay)
    (image,) = near(w0, "near1", False)
    q1, w1, scal, pay = call(
        functools.partial(second_body, **sizes),
        [field, field, scalars, message],
        arrays("s", leaf_sizes) + arrays("v", recv, image, q0, w0, scal, u1, u2)
        + arrays("h", v1, v2),
        scratch=pair_space, flops=small, name="second",
    )
    recv = exchange(pay)
    image, inverse = near(w1, "near2", True)
    q2, scal, pay = call(
        functools.partial(third_body, **sizes),
        [field, scalars, ("v", shaped(num, 1, LANES))],
        arrays("s", leaf_sizes) + arrays("v", recv, image, q0, q1, w0, w1, scal, u1, u2),
        flops=small, name="third",
    )
    recv = exchange(pay)
    (out,) = call(
        last_body, [field], arrays("v", recv, q0, q1, q2, scal, inverse), flops=small, name="last"
    )
    return out


def solution(mesh):
    in_specs = (
        P(None, AXES),
        P(None, AXES),
        P(AXES, None),
        P(AXES),
        P(),
        P(),
        P(None, None, AXES),
        P(None, None, AXES),
    )
    return jax.shard_map(
        per_device, mesh=mesh, in_specs=in_specs, out_specs=P(None, AXES), check_vma=False
    )
```

```python
import functools
import math

import jax
import jax.numpy as jnp
from jax import lax
from jax.experimental import pallas as pl
from jax.experimental.pallas import tpu as pltpu
from jax.sharding import PartitionSpec as P

AXES = ("gx", "gy")
LANES = 128
TILE = 256
EPSILON = 1e-06
DISTANCE_SCALE = math.sqrt(3.0) / math.log(2.0)
LN2 = math.log(2.0)
f32 = jnp.float32
bf16 = jnp.bfloat16


def split(x, parts):
    pieces = []
    for part in range(parts):
        piece = x.astype(bf16)
        pieces.append(piece)
        if part + 1 < parts:
            x = x - piece.astype(f32)
    return pieces


def dot(a, b):
    return lax.dot_general(a, b, (((1,), (0,)), ((), ())), preferred_element_type=f32)


def dot_nt(a, b):
    return lax.dot_general(a, b, (((1,), (1,)), ((), ())), preferred_element_type=f32)


def live_row(size, length):
    return lax.broadcasted_iota(jnp.int32, (1, length), 1) < size


def levels_of(num, levels):
    me = lax.axis_index("gx") * lax.axis_size("gy") + lax.axis_index("gy")
    apart = lax.broadcasted_iota(jnp.int32, (num, 1), 0) ^ me
    level = jnp.full((num, 1), -1, jnp.int32)
    for bit in range(levels):
        level = level + (apart >= (1 << bit)).astype(jnp.int32)
    return level


def diagonal(vectors):
    shape = (LANES // vectors, LANES)
    return lax.broadcasted_iota(jnp.int32, shape, 1) // vectors == lax.broadcasted_iota(
        jnp.int32, shape, 0
    )


def slot_mask(vectors, slot):
    shape = (vectors, LANES)
    return (
        lax.broadcasted_iota(jnp.int32, shape, 1)
        == lax.broadcasted_iota(jnp.int32, shape, 0) + slot * vectors
    )


def pack_dots(pairs, vectors):
    rows = jnp.zeros((vectors, LANES), f32)
    for slot, (a, b) in enumerate(pairs):
        total = jnp.sum(a * b, axis=1, keepdims=True)
        rows = jnp.where(slot_mask(vectors, slot), total, rows)
    return jnp.sum(rows, axis=0, keepdims=True)


def unpack_dots(received, count, vectors):
    total = jnp.sum(received, axis=0, keepdims=True)
    out = []
    for slot in range(count):
        chosen = jnp.where(slot_mask(vectors, slot), total, 0.0)
        out.append(jnp.sum(chosen, axis=1, keepdims=True))
    return out


def send_coefs(vector, high, low, pay_ref, dots, levels, rank):
    vectors = vector.shape[0]
    group = LANES // vectors
    num = pay_ref.shape[0]
    first, second = split(vector, 2)
    wide = jnp.concatenate([first] * group + [second] * group, axis=0)
    both = dot_nt(high, wide) + dot_nt(low, wide)
    both = both[:, :LANES] + both[:, LANES:]
    mask = diagonal(vectors)
    level = levels_of(num, levels)
    for block in range(rank // group):
        rows = jnp.zeros((num, LANES), f32)
        for lev in range(levels):
            start = lev * rank + block * group
            piece = jnp.where(mask, both[start : start + group], 0.0)
            rows = jnp.where(level == lev, jnp.sum(piece, axis=0, keepdims=True), rows)
        pay_ref[:, 0, block * LANES : (block + 1) * LANES] = rows
    pay_ref[:, 0, rank * vectors :] = jnp.broadcast_to(dots, (num, LANES))


def receive_coefs(recv_ref, vectors, levels, rank):
    num = recv_ref.shape[0]
    group = LANES // vectors
    mask = diagonal(vectors)
    level = levels_of(num, levels)
    pieces = []
    for lev in range(levels):
        for block in range(rank // group):
            part = recv_ref[:, 0, block * LANES : (block + 1) * LANES]
            total = jnp.sum(jnp.where(level == lev, part, 0.0), axis=0, keepdims=True)
            pieces.append(jnp.where(mask, jnp.broadcast_to(total, mask.shape), 0.0))
    flipped = jnp.concatenate(pieces, axis=0).T
    out = flipped[:vectors]
    for row in range(1, group):
        out = out + flipped[row * vectors : (row + 1) * vectors]
    return out


def expand(coefs, high, low):
    vectors = coefs.shape[0]
    stacked = jnp.concatenate(split(coefs, 3), axis=0)
    out = dot(stacked, high) + dot(stacked, low)
    return out[:vectors] + out[vectors : 2 * vectors] + out[2 * vectors :]


def one_hot(row, length):
    width = row.shape[1]
    steps = lax.broadcasted_iota(jnp.int32, (TILE, width), 0).astype(f32).astype(bf16)
    pieces = []
    for base in range(0, length, TILE):
        local = (row - base).astype(f32)
        local = jnp.broadcast_to(local, (TILE, width)).astype(bf16)
        pieces.append(jnp.where(steps == local, jnp.ones((), bf16), jnp.zeros((), bf16)))
    return jnp.concatenate(pieces, axis=0)


def start_body(
    sizes_ref, scales_hbm, order_hbm, rhs_hbm, coords_hbm, v_hbm,
    start_ref, points_ref, pay_ref,
    scales_ref, order_ref, rhs_ref, coords_ref, pad_ref, v_ref, sem, *, levels, rank,
):
    loads = [
        pltpu.make_async_copy(source, target, sem.at[n])
        for n, (source, target) in enumerate(
            [
                (scales_hbm, scales_ref),
                (order_hbm, order_ref),
                (rhs_hbm, rhs_ref),
                (coords_hbm, coords_ref),
                (v_hbm, v_ref),
            ]
        )
    ]
    for load in loads:
        load.start()
    vectors, length = rhs_ref.shape
    dims = coords_ref.shape[0]
    pad_ref[...] = jnp.zeros(pad_ref.shape, f32)
    for load in loads[:4]:
        load.wait()
    pad_ref[:dims, :] = coords_ref[...]
    stacked = jnp.concatenate(
        [p.astype(f32) for p in split(rhs_ref[...], 3)]
        + [p.astype(f32) for p in split(pad_ref[...], 3)],
        axis=0,
    ).astype(bf16)
    rows = pad_ref.shape[0]
    row_id = lax.broadcasted_iota(jnp.int32, (rows, 1), 0)
    scale = jnp.zeros((rows, 1), f32)
    for dim in range(dims):
        scale = jnp.where(row_id == dim, scales_ref[dim] * DISTANCE_SCALE, scale)
    for base in range(0, length, TILE):
        chosen = dot(stacked, one_hot(order_ref[:, base : base + TILE], length))
        lane = base + lax.broadcasted_iota(jnp.int32, (1, TILE), 1)
        value = chosen[:vectors] + chosen[vectors : 2 * vectors] + chosen[2 * vectors : 3 * vectors]
        start_ref[:, base : base + TILE] = jnp.where(lane < sizes_ref[0], value, 0.0)
        rest = chosen[3 * vectors :]
        value = rest[:rows] + rest[rows : 2 * rows] + rest[2 * rows :]
        points_ref[:, base : base + TILE] = value * scale

    @stage(sizes_ref[0])
    def _():
        loads[4].wait()
        high, low = split(v_ref[...], 2)
        start = start_ref[...]
        dots = pack_dots([(start, start)], vectors)
        send_coefs(start, high, low, pay_ref, dots, levels, rank)


def blocks_of(ref, first, count):
    return jnp.concatenate(
        [ref[(first + n) * TILE : (first + n + 1) * TILE, :] for n in range(count)], axis=1
    )


def stage(value):
    return pl.when(value > -1)


def add_panel(stacked, high_ref, low_ref, acc_ref, base, offset):
    width = acc_ref.shape[1] - base
    own = stacked[:, base : base + TILE]
    first = offset // LANES
    for half in (high_ref, low_ref):
        panel = blocks_of(half, first, width // LANES)
        acc_ref[:, base:] += dot(own, panel)
        if width > TILE:
            acc_ref[:, base : base + TILE] += dot_nt(stacked[:, base + TILE :], panel[:, TILE:])


def panel_rows(ref, offset, width):
    return ref.at[pl.ds(offset // LANES * TILE, width // LANES * TILE), :]


def finish(acc_ref, noise_ref, vector):
    vectors = vector.shape[0]
    out = acc_ref[...]
    out = out[:vectors] + out[vectors : 2 * vectors] + out[2 * vectors :]
    return LN2 * out + noise_ref[0] * vector


def panels(length):
    offset = 0
    for base in range(0, length, TILE):
        yield base, offset, length - base
        offset += length - base


def build_body(
    noise_ref, points_ref, start_ref, u_hbm, high_hbm, low_hbm, image_ref, u1_ref, u2_ref,
    u_ref, wide_ref, high_ref, low_ref, acc_ref, sem, *, dims,
):
    length = points_ref.shape[1]
    step = 16
    load = pltpu.make_async_copy(u_hbm, u_ref, sem.at[0])
    load.start()
    columns = points_ref[...].T
    for dim in range(dims):
        wide_ref[dim] = jnp.broadcast_to(columns[:, dim : dim + 1], (length, LANES))
    start = start_ref[...]
    stacked = jnp.concatenate(split(start, 3), axis=0)
    acc_ref[...] = jnp.zeros(acc_ref.shape, f32)
    copies = []
    for base, offset, width in panels(length):
        for row in range(0, TILE, step):
            column = [wide_ref[dim, base + row : base + row + step, :] for dim in range(dims)]
            for lane in range(base, length, LANES):
                square = None
                for dim in range(dims):
                    differ = column[dim] - points_ref[dim : dim + 1, lane : lane + LANES]
                    square = differ * differ if square is None else square + differ * differ
                square = jnp.maximum(square, 1e-30)
                distance = square * lax.rsqrt(square)
                value = (1.0 / LN2 + distance) * jnp.exp2(-distance)
                high, low = split(value, 2)
                place = (offset + lane - base) // LANES * TILE + row
                high_ref[place : place + step, :] = high
                low_ref[place : place + step, :] = low
        for source, target in ((high_ref, high_hbm), (low_ref, low_hbm)):
            copy = pltpu.make_async_copy(
                panel_rows(source, offset, width),
                panel_rows(target, offset, width),
                sem.at[1 + len(copies)],
            )
            copy.start()
            copies.append(copy)
        add_panel(stacked, high_ref, low_ref, acc_ref, base, offset)
    image_ref[...] = finish(acc_ref, noise_ref, start)

    @stage(noise_ref[0])
    def _():
        load.wait()
        high, low = split(u_ref[...], 2)
        u1_ref[...] = high
        u2_ref[...] = low

    @stage(noise_ref[0])
    def _():
        for copy in copies:
            copy.wait()


def near_body(
    noise_ref, vector_ref, high_hbm, low_hbm, *refs, order
):
    if order:
        order_ref, image_ref, inverse_ref, high_ref, low_ref, acc_ref, sem = refs
    else:
        image_ref, high_ref, low_ref, acc_ref, sem = refs
    vector = vector_ref[...]
    length = vector.shape[1]
    copies = []
    for base, offset, width in panels(length):
        for source, target in ((high_hbm, high_ref), (low_hbm, low_ref)):
            copy = pltpu.make_async_copy(
                panel_rows(source, offset, width),
                panel_rows(target, offset, width),
                sem.at[len(copies)],
            )
            copies.append(copy)
    ahead = 4
    for copy in copies[:ahead]:
        copy.start()
    stacked = jnp.concatenate(split(vector, 3), axis=0)
    acc_ref[...] = jnp.zeros(acc_ref.shape, f32)
    if order:
        inverse_ref[...] = inverse_of(order_ref)
    for number, (base, offset, width) in enumerate(panels(length)):

        @stage(noise_ref[0])
        def _(number=number, base=base, offset=offset):
            for copy in copies[2 * number : 2 * number + 2]:
                copy.wait()
            for copy in copies[2 * number + ahead : 2 * number + ahead + 2]:
                copy.start()
            add_panel(stacked, high_ref, low_ref, acc_ref, base, offset)

    image_ref[...] = finish(acc_ref, noise_ref, vector)


def inverse_of(order_ref):
    length = order_ref.shape[1]
    place = lax.broadcasted_iota(jnp.int32, (8, TILE), 1).astype(f32)
    row_id = lax.broadcasted_iota(jnp.int32, (8, TILE), 0)
    total = jnp.zeros((8, length), f32)
    for base in range(0, length, TILE):
        weights = jnp.where(row_id == 0, place, float(base // TILE))
        hot = one_hot(order_ref[:, base : base + TILE], length)
        total = total + dot_nt(weights.astype(bf16), hot)
    return (total[0:1] + total[1:2] * float(TILE)).astype(jnp.int32)


def first_body(
    sizes_ref, recv_ref, image_ref, start_ref, u1_ref, u2_ref, v_hbm,
    q0_ref, w0_ref, scal_ref, pay_ref, v_ref, sem, *, levels, rank,
):
    load = pltpu.make_async_copy(v_hbm, v_ref, sem.at[0])
    load.start()
    vectors, length = start_ref.shape
    live = live_row(sizes_ref[0], length)
    (norm,) = unpack_dots(recv_ref[:, 0, rank * vectors :], 1, vectors)
    beta = jnp.sqrt(norm + EPSILON)
    inverse = 1.0 / beta
    distant = expand(receive_coefs(recv_ref, vectors, levels, rank), u1_ref[...], u2_ref[...])
    w0 = jnp.where(live, image_ref[...] + distant, 0.0) * inverse
    q0 = start_ref[...] * inverse
    q0_ref[...] = q0
    w0_ref[...] = w0
    scal_ref[...] = jnp.broadcast_to(beta, scal_ref.shape)
    dots = pack_dots([(q0, q0), (q0, w0), (w0, w0)], vectors)

    @stage(sizes_ref[0])
    def _():
        load.wait()
        high, low = split(v_ref[...], 2)
        send_coefs(w0_ref[...], high, low, pay_ref, dots, levels, rank)


def put_scalars(scal_ref, values):
    lane = lax.broadcasted_iota(jnp.int32, scal_ref.shape, 1)
    out = jnp.zeros(scal_ref.shape, f32)
    for slot, value in enumerate(values):
        out = jnp.where(lane == slot, value, out)
    scal_ref[...] = out


def get_scalars(scal_ref, count):
    return [scal_ref[:, slot : slot + 1] for slot in range(count)]


def second_body(
    sizes_ref, recv_ref, image_ref, q0_ref, w0_ref, old_ref, u1_ref, u2_ref, v_hbm,
    q1_ref, w1_ref, scal_ref, pay_ref, v_ref, sem, *, levels, rank,
):
    load = pltpu.make_async_copy(v_hbm, v_ref, sem.at[0])
    load.start()
    vectors, length = q0_ref.shape
    live = live_row(sizes_ref[0], length)
    (beta,) = get_scalars(old_ref, 1)
    g00, h00, norm = unpack_dots(recv_ref[:, 0, rank * vectors :], 3, vectors)
    rest = norm - 2.0 * h00 * h00 + h00 * h00 * g00
    h10 = jnp.sqrt(jnp.maximum(rest, 0.0) + EPSILON)
    inverse = 1.0 / h10
    put_scalars(scal_ref, [beta, g00, h00, h10])
    distant = expand(receive_coefs(recv_ref, vectors, levels, rank), u1_ref[...], u2_ref[...])
    w0 = w0_ref[...]
    q0 = q0_ref[...]
    q1 = (w0 - h00 * q0) * inverse
    w1 = (jnp.where(live, image_ref[...] + distant, 0.0) - h00 * w0) * inverse
    q1_ref[...] = q1
    w1_ref[...] = w1
    dots = pack_dots([(q0, w1), (q1, w1), (w1, w1), (q0, q1), (q1, q1)], vectors)

    @stage(sizes_ref[0])
    def _():
        load.wait()
        high, low = split(v_ref[...], 2)
        send_coefs(w1_ref[...], high, low, pay_ref, dots, levels, rank)


def third_body(
    sizes_ref, recv_ref, image_ref, q0_ref, q1_ref, w0_ref, w1_ref, old_ref, u1_ref, u2_ref,
    q2_ref, scal_ref, pay_ref, *, levels, rank,
):
    vectors, length = q0_ref.shape
    live = live_row(sizes_ref[0], length)
    beta, g00, h00, h10 = get_scalars(old_ref, 4)
    h01, h11, norm, g01, g11 = unpack_dots(recv_ref[:, 0, rank * vectors :], 5, vectors)
    rest = (
        norm - 2.0 * (h01 * h01 + h11 * h11)
        + (h01 * h01 * g00 + h11 * h11 * g11 + 2.0 * h01 * h11 * g01)
    )
    h21 = jnp.sqrt(jnp.maximum(rest, 0.0) + EPSILON)
    inverse = 1.0 / h21
    put_scalars(scal_ref, [beta, g00, h00, h10, g01, g11, h01, h11, h21])
    distant = expand(receive_coefs(recv_ref, vectors, levels, rank), u1_ref[...], u2_ref[...])
    w0 = w0_ref[...]
    w1 = w1_ref[...]
    q0 = q0_ref[...]
    q1 = q1_ref[...]
    q2 = (w1 - h01 * q0 - h11 * q1) * inverse
    image = jnp.where(live, image_ref[...] + distant, 0.0)
    w2 = (image - h01 * w0 - h11 * w1) * inverse
    q2_ref[...] = q2
    dots = pack_dots(
        [(q0, w2), (q1, w2), (q2, w2), (w2, w2), (q0, q2), (q1, q2), (q2, q2)], vectors
    )
    num, _, width = pay_ref.shape
    pay_ref[:, 0, :] = jnp.broadcast_to(dots, (num, width))


def least_squares(columns, beta):
    count_cols = len(columns)
    cosines = []
    sines = []
    target = [beta] + [jnp.zeros_like(beta)] * count_cols
    upper = []
    for column_idx in range(count_cols):
        entries = list(columns[column_idx])
        for row_idx in range(column_idx):
            first_val = entries[row_idx]
            second_val = entries[row_idx + 1]
            entries[row_idx] = cosines[row_idx] * first_val + sines[row_idx] * second_val
            entries[row_idx + 1] = -sines[row_idx] * first_val + cosines[row_idx] * second_val
        first_val = entries[column_idx]
        second_val = entries[column_idx + 1]
        radius = jnp.sqrt(first_val * first_val + second_val * second_val)
        cosines.append(first_val / radius)
        sines.append(second_val / radius)
        entries[column_idx] = radius
        carried = target[column_idx]
        target[column_idx] = cosines[column_idx] * carried
        target[column_idx + 1] = -sines[column_idx] * carried
        upper.append(entries[: column_idx + 1])
    weights = [None] * count_cols
    for column_idx in reversed(range(count_cols)):
        accum = target[column_idx]
        for later_idx in range(column_idx + 1, count_cols):
            accum = accum - upper[later_idx][column_idx] * weights[later_idx]
        weights[column_idx] = accum / upper[column_idx][column_idx]
    return weights


def last_body(recv_ref, q0_ref, q1_ref, q2_ref, old_ref, inverse_ref, out_ref):
    vectors, length = q0_ref.shape
    beta, g00, h00, h10, g01, g11, h01, h11, h21 = get_scalars(old_ref, 9)
    h02, h12, h22, norm, g02, g12, g22 = unpack_dots(recv_ref[:, 0, :], 7, vectors)
    rest = (
        norm - 2.0 * (h02 * h02 + h12 * h12 + h22 * h22)
        + (h02 * h02 * g00 + h12 * h12 * g11 + h22 * h22 * g22)
        + 2.0 * (h02 * h12 * g01 + h02 * h22 * g02 + h12 * h22 * g12)
    )
    h32 = jnp.sqrt(jnp.maximum(rest, 0.0) + EPSILON)
    y0, y1, y2 = least_squares([[h00, h10], [h01, h11, h21], [h02, h12, h22, h32]], beta)
    solved = y0 * q0_ref[...] + y1 * q1_ref[...] + y2 * q2_ref[...]
    stacked = jnp.concatenate(split(solved, 3), axis=0)
    for base in range(0, length, TILE):
        placed = dot(stacked, one_hot(inverse_ref[:, base : base + TILE], length))
        out_ref[:, base : base + TILE] = (
            placed[:vectors] + placed[vectors : 2 * vectors] + placed[2 * vectors :]
        )


def call(body, outs, args, scratch=(), flops=0, limit=20000, name=None):
    spaces = dict(s=pltpu.SMEM, v=pltpu.VMEM, h=pltpu.HBM)
    total = sum(math.prod(a.shape) * a.dtype.itemsize for _, a in list(args) + list(outs))
    return pl.pallas_call(
        body,
        out_shape=[pltpu.HBM(a.shape, a.dtype) if m == "h" else a for m, a in outs],
        in_specs=[pl.BlockSpec(memory_space=spaces[m]) for m, _ in args],
        out_specs=[pl.BlockSpec(memory_space=spaces[m]) for m, _ in outs],
        scratch_shapes=list(scratch),
        compiler_params=pltpu.CompilerParams(vmem_limit_bytes=limit * 1024),
        cost_estimate=pl.CostEstimate(flops=flops, bytes_accessed=total, transcendentals=0),
        name=name,
    )(*[pltpu.with_memory_space_constraint(a, pltpu.HBM) if m == "h" else a for m, a in args])


def exchange(payload):
    return lax.all_to_all(payload, AXES, 0, 0, tiled=True)


def per_device(
    coordinates, rhs, leaf_order, leaf_sizes, inverse_scales, noise_var, u_factors, v_factors
):
    vectors, length = rhs.shape
    dims = coordinates.shape[0]
    levels, rank, _ = u_factors.shape
    num = lax.axis_size("gx") * lax.axis_size("gy")
    blocks = length // TILE
    packed = TILE * (blocks * (blocks + 1) // 2)
    padded = -(-dims // 8) * 8
    u_flat = u_factors.reshape(levels * rank, length)
    v_flat = v_factors.reshape(levels * rank, length)

    def shaped(*shape, dtype=f32):
        return jax.ShapeDtypeStruct(shape, dtype)

    field = ("v", shaped(vectors, length))
    factor = shaped(levels * rank, length, dtype=bf16)
    scalars = ("v", shaped(vectors, LANES))
    message = ("v", shaped(num, 1, rank * vectors + LANES))
    panel = shaped(packed // LANES * TILE, LANES, dtype=bf16)
    acc = pltpu.VMEM((3 * vectors, length), f32)
    panel_space = pltpu.VMEM((packed // LANES * TILE, LANES), bf16)
    whole_space = pltpu.VMEM((levels * rank, length), f32)
    sizes = dict(levels=levels, rank=rank)
    small = 2 * levels * rank * length * 256

    def arrays(memory, *values):
        return [(memory, value) for value in values]

    start, points, pay = call(
        functools.partial(start_body, **sizes),
        [field, ("v", shaped(padded, length)), message],
        arrays("s", leaf_sizes)
        + arrays("h", inverse_scales, leaf_order, rhs, coordinates, v_flat),
        scratch=[
            pltpu.SMEM((dims,), f32),
            pltpu.VMEM((1, length), jnp.int32),
            pltpu.VMEM((vectors, length), f32),
            pltpu.VMEM((dims, length), f32),
            pltpu.VMEM((padded, length), f32),
            whole_space,
            pltpu.SemaphoreType.DMA((5,)),
        ],
        flops=small, name="start",
    )
    recv = exchange(pay)
    k1, k2, image, u1, u2 = call(
        functools.partial(build_body, dims=dims),
        [("h", panel), ("h", panel), field, ("v", factor), ("v", factor)],
        arrays("s", noise_var) + arrays("v", points, start) + arrays("h", u_flat),
        scratch=[
            whole_space,
            pltpu.VMEM((dims, length, LANES), f32),
            panel_space,
            panel_space,
            acc,
            pltpu.SemaphoreType.DMA((1 + 2 * blocks,)),
        ],
        flops=2 * length * length * 256, limit=40000, name="build",
    )

    def near(vector, name, order):
        return call(
            functools.partial(near_body, order=order),
            [field] + ([("v", shaped(1, length, dtype=jnp.int32))] if order else []),
            arrays("s", noise_var) + arrays("v", vector) + arrays("h", k1, k2)
            + (arrays("v", leaf_order) if order else []),
            scratch=[panel_space, panel_space, acc, pltpu.SemaphoreType.DMA((2 * blocks,))],
            flops=2 * length * length * 128, limit=30000, name=name,
        )

    whole_load = [whole_space, pltpu.SemaphoreType.DMA((1,))]
    q0, w0, scal, pay = call(
        functools.partial(first_body, **sizes),
        [field, field, scalars, message],
        arrays("s", leaf_sizes) + arrays("v", recv, image, start, u1, u2) + arrays("h", v_flat),
        scratch=whole_load, flops=small, name="first",
    )
    recv = exchange(pay)
    (image,) = near(w0, "near1", False)
    q1, w1, scal, pay = call(
        functools.partial(second_body, **sizes),
        [field, field, scalars, message],
        arrays("s", leaf_sizes) + arrays("v", recv, image, q0, w0, scal, u1, u2)
        + arrays("h", v_flat),
        scratch=whole_load, flops=small, name="second",
    )
    recv = exchange(pay)
    image, inverse = near(w1, "near2", True)
    q2, scal, pay = call(
        functools.partial(third_body, **sizes),
        [field, scalars, ("v", shaped(num, 1, LANES))],
        arrays("s", leaf_sizes) + arrays("v", recv, image, q0, q1, w0, w1, scal, u1, u2),
        flops=small, name="third",
    )
    recv = exchange(pay)
    (out,) = call(
        last_body, [field], arrays("v", recv, q0, q1, q2, scal, inverse), flops=small, name="last"
    )
    return out


def solution(mesh):
    in_specs = (
        P(None, AXES),
        P(None, AXES),
        P(AXES, None),
        P(AXES),
        P(),
        P(),
        P(None, None, AXES),
        P(None, None, AXES),
    )
    return jax.shard_map(
        per_device, mesh=mesh, in_specs=in_specs, out_specs=P(None, AXES), check_vma=False
    )
```

```python
import functools
import math

import jax
import jax.numpy as jnp
from jax import lax
from jax.experimental import pallas as pl
from jax.experimental.pallas import tpu as pltpu
from jax.sharding import PartitionSpec as P

AXES = ("gx", "gy")
LANES = 128
TILE = 256
EPSILON = 1e-06
DISTANCE_SCALE = math.sqrt(3.0) / math.log(2.0)
LN2 = math.log(2.0)
f32 = jnp.float32
bf16 = jnp.bfloat16


def split(x, parts):
    pieces = []
    for part in range(parts):
        piece = x.astype(bf16)
        pieces.append(piece)
        if part + 1 < parts:
            x = x - piece.astype(f32)
    return pieces


def dot(a, b):
    return lax.dot_general(a, b, (((1,), (0,)), ((), ())), preferred_element_type=f32)


def dot_nt(a, b):
    return lax.dot_general(a, b, (((1,), (1,)), ((), ())), preferred_element_type=f32)


def dot_halves(a, high, low):
    return dot(jnp.concatenate([a, a], axis=1), jnp.concatenate([high, low], axis=0))


def live_row(size, length):
    return lax.broadcasted_iota(jnp.int32, (1, length), 1) < size


def levels_of(num, levels):
    me = lax.axis_index("gx") * lax.axis_size("gy") + lax.axis_index("gy")
    apart = lax.broadcasted_iota(jnp.int32, (num, 1), 0) ^ me
    level = jnp.full((num, 1), -1, jnp.int32)
    for bit in range(levels):
        level = level + (apart >= (1 << bit)).astype(jnp.int32)
    return level


def diagonal(vectors):
    shape = (LANES // vectors, LANES)
    return lax.broadcasted_iota(jnp.int32, shape, 1) // vectors == lax.broadcasted_iota(
        jnp.int32, shape, 0
    )


def slot_mask(vectors, slot):
    shape = (vectors, LANES)
    return (
        lax.broadcasted_iota(jnp.int32, shape, 1)
        == lax.broadcasted_iota(jnp.int32, shape, 0) + slot * vectors
    )


def pack_dots(pairs, vectors):
    rows = jnp.zeros((vectors, LANES), f32)
    for slot, (a, b) in enumerate(pairs):
        total = jnp.sum(a * b, axis=1, keepdims=True)
        rows = jnp.where(slot_mask(vectors, slot), total, rows)
    return jnp.sum(rows, axis=0, keepdims=True)


def unpack_dots(received, count, vectors):
    total = jnp.sum(received, axis=0, keepdims=True)
    out = []
    for slot in range(count):
        chosen = jnp.where(slot_mask(vectors, slot), total, 0.0)
        out.append(jnp.sum(chosen, axis=1, keepdims=True))
    return out


def send_coefs(vector, high, low, pay_ref, dots, levels, rank):
    vectors = vector.shape[0]
    group = LANES // vectors
    num = pay_ref.shape[0]
    first, second = split(vector, 2)
    wide = jnp.concatenate([first] * group + [second] * group, axis=0)
    both = dot_nt(high, wide) + dot_nt(low, wide)
    both = both[:, :LANES] + both[:, LANES:]
    mask = diagonal(vectors)
    level = levels_of(num, levels)
    for block in range(rank // group):
        rows = jnp.zeros((num, LANES), f32)
        for lev in range(levels):
            start = lev * rank + block * group
            piece = jnp.where(mask, both[start : start + group], 0.0)
            rows = jnp.where(level == lev, jnp.sum(piece, axis=0, keepdims=True), rows)
        pay_ref[:, 0, block * LANES : (block + 1) * LANES] = rows
    pay_ref[:, 0, rank * vectors :] = jnp.broadcast_to(dots, (num, LANES))


def receive_coefs(recv_ref, vectors, levels, rank):
    num = recv_ref.shape[0]
    group = LANES // vectors
    mask = diagonal(vectors)
    level = levels_of(num, levels)
    pieces = []
    for lev in range(levels):
        for block in range(rank // group):
            part = recv_ref[:, 0, block * LANES : (block + 1) * LANES]
            total = jnp.sum(jnp.where(level == lev, part, 0.0), axis=0, keepdims=True)
            pieces.append(jnp.where(mask, jnp.broadcast_to(total, mask.shape), 0.0))
    flipped = jnp.concatenate(pieces, axis=0).T
    out = flipped[:vectors]
    for row in range(1, group):
        out = out + flipped[row * vectors : (row + 1) * vectors]
    return out


def expand(coefs, high, low):
    vectors = coefs.shape[0]
    stacked = jnp.concatenate(split(coefs, 3), axis=0)
    out = dot(stacked, high) + dot(stacked, low)
    return out[:vectors] + out[vectors : 2 * vectors] + out[2 * vectors :]


def one_hot(row, length):
    width = row.shape[1]
    steps = lax.broadcasted_iota(jnp.int32, (TILE, width), 0).astype(f32).astype(bf16)
    pieces = []
    for base in range(0, length, TILE):
        local = (row - base).astype(f32)
        local = jnp.broadcast_to(local, (TILE, width)).astype(bf16)
        pieces.append(jnp.where(steps == local, jnp.ones((), bf16), jnp.zeros((), bf16)))
    return jnp.concatenate(pieces, axis=0)


def start_body(
    sizes_ref, noise_ref, scales_hbm, order_hbm, rhs_hbm, coords_hbm, v_hbm,
    start_ref, points_ref, pay_ref,
    scales_ref, order_ref, rhs_ref, coords_ref, pad_ref, v_ref, sem, *, levels, rank,
):
    loads = [
        pltpu.make_async_copy(source, target, sem.at[n])
        for n, (source, target) in enumerate(
            [
                (scales_hbm, scales_ref),
                (order_hbm, order_ref),
                (rhs_hbm, rhs_ref),
                (coords_hbm, coords_ref),
                (v_hbm, v_ref),
            ]
        )
    ]
    for load in loads:
        load.start()
    vectors, length = rhs_ref.shape
    dims = coords_ref.shape[0]
    pad_ref[...] = jnp.zeros(pad_ref.shape, f32)
    for load in loads[:4]:
        load.wait()
    pad_ref[:dims, :] = coords_ref[...]
    stacked = jnp.concatenate(
        [p.astype(f32) for p in split(rhs_ref[...], 3)]
        + [p.astype(f32) for p in split(pad_ref[...], 3)],
        axis=0,
    ).astype(bf16)
    rows = pad_ref.shape[0]
    row_id = lax.broadcasted_iota(jnp.int32, (rows, 1), 0)
    scale = jnp.zeros((rows, 1), f32)
    for dim in range(dims):
        scale = jnp.where(row_id == dim, scales_ref[dim] * DISTANCE_SCALE, scale)
    for base in range(0, length, TILE):
        chosen = dot(stacked, one_hot(order_ref[:, base : base + TILE], length))
        lane = base + lax.broadcasted_iota(jnp.int32, (1, TILE), 1)
        value = chosen[:vectors] + chosen[vectors : 2 * vectors] + chosen[2 * vectors : 3 * vectors]
        start_ref[:, base : base + TILE] = jnp.where(lane < sizes_ref[0], value, 0.0)
        rest = chosen[3 * vectors :]
        value = rest[:rows] + rest[rows : 2 * rows] + rest[2 * rows :]
        points_ref[:, base : base + TILE] = jnp.where(row_id == dims, noise_ref[0], value * scale)

    @stage(sizes_ref[0])
    def _():
        loads[4].wait()
        high, low = split(v_ref[...], 2)
        start = start_ref[...]
        dots = pack_dots([(start, start)], vectors)
        send_coefs(start, high, low, pay_ref, dots, levels, rank)


def blocks_of(ref, first, count):
    return jnp.concatenate(
        [ref[(first + n) * TILE : (first + n + 1) * TILE, :] for n in range(count)], axis=1
    )


def stage(value):
    return pl.when(value > -1)


def add_panel(stacked, high_ref, low_ref, acc_ref, base, offset):
    width = acc_ref.shape[1] - base
    own = stacked[:, base : base + TILE]
    first = offset // LANES
    high = blocks_of(high_ref, first, width // LANES)
    low = blocks_of(low_ref, first, width // LANES)
    acc_ref[:, base:] += dot_halves(own, high, low)
    if width > TILE:
        rest = stacked[:, base + TILE :]
        acc_ref[:, base : base + TILE] += dot_nt(
            jnp.concatenate([rest, rest], axis=1),
            jnp.concatenate([high[:, TILE:], low[:, TILE:]], axis=1),
        )


def panel_rows(ref, offset, width):
    return ref.at[pl.ds(offset // LANES * TILE, width // LANES * TILE), :]


def finish(acc_ref, points_ref, vector, dims):
    vectors = vector.shape[0]
    out = acc_ref[...]
    out = out[:vectors] + out[vectors : 2 * vectors] + out[2 * vectors :]
    return LN2 * out + points_ref[dims : dims + 1, :] * vector


def panels(length):
    offset = 0
    for base in range(0, length, TILE):
        yield base, offset, length - base
        offset += length - base


def build_body(
    sizes_ref, points_ref, start_ref, u_hbm, high_hbm, low_hbm, image_ref, u1_ref, u2_ref,
    u_ref, wide_ref, high_ref, low_ref, acc_ref, sem, *, dims,
):
    length = points_ref.shape[1]
    step = 16
    load = pltpu.make_async_copy(u_hbm, u_ref, sem.at[0])
    load.start()
    columns = points_ref[...].T
    for dim in range(dims):
        wide_ref[dim] = jnp.broadcast_to(columns[:, dim : dim + 1], (length, LANES))
    start = start_ref[...]
    stacked = jnp.concatenate(split(start, 3), axis=0)
    acc_ref[...] = jnp.zeros(acc_ref.shape, f32)
    copies = []
    for base, offset, width in panels(length):
        for row in range(0, TILE, step):
            column = [wide_ref[dim, base + row : base + row + step, :] for dim in range(dims)]
            for lane in range(base, length, LANES):
                square = None
                for dim in range(dims):
                    differ = column[dim] - points_ref[dim : dim + 1, lane : lane + LANES]
                    square = differ * differ if square is None else square + differ * differ
                square = jnp.maximum(square, 1e-30)
                distance = square * lax.rsqrt(square)
                value = (1.0 / LN2 + distance) * jnp.exp2(-distance)
                high, low = split(value, 2)
                place = (offset + lane - base) // LANES * TILE + row
                high_ref[place : place + step, :] = high
                low_ref[place : place + step, :] = low
        for source, target in ((high_ref, high_hbm), (low_ref, low_hbm)):
            copy = pltpu.make_async_copy(
                panel_rows(source, offset, width),
                panel_rows(target, offset, width),
                sem.at[1 + len(copies)],
            )
            copy.start()
            copies.append(copy)
        add_panel(stacked, high_ref, low_ref, acc_ref, base, offset)

    @stage(sizes_ref[0])
    def _():
        image_ref[...] = finish(acc_ref, points_ref, start, dims)
        load.wait()
        high, low = split(u_ref[...], 2)
        u1_ref[...] = high
        u2_ref[...] = low

    @stage(sizes_ref[0])
    def _():
        for copy in copies:
            copy.wait()


def near_body(
    sizes_ref, points_ref, vector_ref, high_hbm, low_hbm, image_ref,
    high_ref, low_ref, acc_ref, sem, *, dims,
):
    vector = vector_ref[...]
    length = vector.shape[1]
    copies = []
    for base, offset, width in panels(length):
        for source, target in ((high_hbm, high_ref), (low_hbm, low_ref)):
            copy = pltpu.make_async_copy(
                panel_rows(source, offset, width),
                panel_rows(target, offset, width),
                sem.at[len(copies)],
            )
            copies.append(copy)
    ahead = 4
    for copy in copies[:ahead]:
        copy.start()
    stacked = jnp.concatenate(split(vector, 3), axis=0)
    acc_ref[...] = jnp.zeros(acc_ref.shape, f32)
    for number, (base, offset, width) in enumerate(panels(length)):

        @stage(sizes_ref[0])
        def _(number=number, base=base, offset=offset):
            for copy in copies[2 * number : 2 * number + 2]:
                copy.wait()
            for copy in copies[2 * number + ahead : 2 * number + ahead + 2]:
                copy.start()
            add_panel(stacked, high_ref, low_ref, acc_ref, base, offset)

    @stage(sizes_ref[0])
    def _():
        image_ref[...] = finish(acc_ref, points_ref, vector, dims)


def place_body(order_ref, *refs):
    count = (len(refs) - 1) // 2
    sources, targets, acc_ref = refs[:count], refs[count : 2 * count], refs[-1]
    vectors, length = sources[0].shape
    stacked = jnp.concatenate([p for ref in sources for p in split(ref[...], 3)], axis=0)
    for base in range(0, length, TILE):
        hot = one_hot(order_ref[:, base : base + TILE], length)
        part = dot_nt(stacked[:, base : base + TILE], hot)
        if base == 0:
            acc_ref[...] = part
        else:
            acc_ref[...] += part
    for number, target in enumerate(targets):
        first = 3 * number * vectors
        pieces = [acc_ref[first + n * vectors : first + (n + 1) * vectors, :] for n in range(3)]
        target[...] = pieces[0] + pieces[1] + pieces[2]


def first_body(
    sizes_ref, recv_ref, image_ref, start_ref, u1_ref, u2_ref, v_hbm,
    q0_ref, w0_ref, scal_ref, pay_ref, v_ref, sem, *, levels, rank,
):
    load = pltpu.make_async_copy(v_hbm, v_ref, sem.at[0])
    load.start()
    vectors, length = start_ref.shape
    live = live_row(sizes_ref[0], length)
    (norm,) = unpack_dots(recv_ref[:, 0, rank * vectors :], 1, vectors)
    beta = jnp.sqrt(norm + EPSILON)
    inverse = 1.0 / beta
    distant = expand(receive_coefs(recv_ref, vectors, levels, rank), u1_ref[...], u2_ref[...])
    w0 = jnp.where(live, image_ref[...] + distant, 0.0) * inverse
    q0 = start_ref[...] * inverse
    q0_ref[...] = q0
    w0_ref[...] = w0
    scal_ref[...] = jnp.broadcast_to(beta, scal_ref.shape)
    dots = pack_dots([(q0, q0), (q0, w0), (w0, w0)], vectors)

    @stage(sizes_ref[0])
    def _():
        load.wait()
        high, low = split(v_ref[...], 2)
        send_coefs(w0_ref[...], high, low, pay_ref, dots, levels, rank)


def put_scalars(scal_ref, values):
    lane = lax.broadcasted_iota(jnp.int32, scal_ref.shape, 1)
    out = jnp.zeros(scal_ref.shape, f32)
    for slot, value in enumerate(values):
        out = jnp.where(lane == slot, value, out)
    scal_ref[...] = out


def get_scalars(scal_ref, count):
    return [scal_ref[:, slot : slot + 1] for slot in range(count)]


def second_body(
    sizes_ref, recv_ref, image_ref, q0_ref, w0_ref, old_ref, u1_ref, u2_ref, v_hbm,
    q1_ref, w1_ref, scal_ref, pay_ref, v_ref, sem, *, levels, rank,
):
    load = pltpu.make_async_copy(v_hbm, v_ref, sem.at[0])
    load.start()
    vectors, length = q0_ref.shape
    live = live_row(sizes_ref[0], length)
    (beta,) = get_scalars(old_ref, 1)
    g00, h00, norm = unpack_dots(recv_ref[:, 0, rank * vectors :], 3, vectors)
    rest = norm - 2.0 * h00 * h00 + h00 * h00 * g00
    h10 = jnp.sqrt(jnp.maximum(rest, 0.0) + EPSILON)
    inverse = 1.0 / h10
    put_scalars(scal_ref, [beta, g00, h00, h10])
    distant = expand(receive_coefs(recv_ref, vectors, levels, rank), u1_ref[...], u2_ref[...])
    w0 = w0_ref[...]
    q0 = q0_ref[...]
    q1 = (w0 - h00 * q0) * inverse
    w1 = (jnp.where(live, image_ref[...] + distant, 0.0) - h00 * w0) * inverse
    q1_ref[...] = q1
    w1_ref[...] = w1
    dots = pack_dots([(q0, w1), (q1, w1), (w1, w1), (q0, q1), (q1, q1)], vectors)

    @stage(sizes_ref[0])
    def _():
        load.wait()
        high, low = split(v_ref[...], 2)
        send_coefs(w1_ref[...], high, low, pay_ref, dots, levels, rank)


def third_body(
    sizes_ref, recv_ref, image_ref, q0_ref, q1_ref, w0_ref, w1_ref, old_ref, u1_ref, u2_ref,
    scal_ref, pay_ref, *, levels, rank,
):
    vectors, length = q0_ref.shape
    live = live_row(sizes_ref[0], length)
    beta, g00, h00, h10 = get_scalars(old_ref, 4)
    h01, h11, norm, g01, g11 = unpack_dots(recv_ref[:, 0, rank * vectors :], 5, vectors)
    rest = (
        norm - 2.0 * (h01 * h01 + h11 * h11)
        + (h01 * h01 * g00 + h11 * h11 * g11 + 2.0 * h01 * h11 * g01)
    )
    h21 = jnp.sqrt(jnp.maximum(rest, 0.0) + EPSILON)
    inverse = 1.0 / h21
    put_scalars(scal_ref, [beta, g00, h00, h10, g01, g11, h01, h11, h21])
    distant = expand(receive_coefs(recv_ref, vectors, levels, rank), u1_ref[...], u2_ref[...])
    w0 = w0_ref[...]
    w1 = w1_ref[...]
    q0 = q0_ref[...]
    q1 = q1_ref[...]
    q2 = (w1 - h01 * q0 - h11 * q1) * inverse
    image = jnp.where(live, image_ref[...] + distant, 0.0)
    w2 = (image - h01 * w0 - h11 * w1) * inverse
    dots = pack_dots(
        [(q0, w2), (q1, w2), (q2, w2), (w2, w2), (q0, q2), (q1, q2), (q2, q2)], vectors
    )
    num, _, width = pay_ref.shape
    pay_ref[:, 0, :] = jnp.broadcast_to(dots, (num, width))


def least_squares(columns, beta):
    count_cols = len(columns)
    cosines = []
    sines = []
    target = [beta] + [jnp.zeros_like(beta)] * count_cols
    upper = []
    for column_idx in range(count_cols):
        entries = list(columns[column_idx])
        for row_idx in range(column_idx):
            first_val = entries[row_idx]
            second_val = entries[row_idx + 1]
            entries[row_idx] = cosines[row_idx] * first_val + sines[row_idx] * second_val
            entries[row_idx + 1] = -sines[row_idx] * first_val + cosines[row_idx] * second_val
        first_val = entries[column_idx]
        second_val = entries[column_idx + 1]
        radius = jnp.sqrt(first_val * first_val + second_val * second_val)
        cosines.append(first_val / radius)
        sines.append(second_val / radius)
        entries[column_idx] = radius
        carried = target[column_idx]
        target[column_idx] = cosines[column_idx] * carried
        target[column_idx + 1] = -sines[column_idx] * carried
        upper.append(entries[: column_idx + 1])
    weights = [None] * count_cols
    for column_idx in reversed(range(count_cols)):
        accum = target[column_idx]
        for later_idx in range(column_idx + 1, count_cols):
            accum = accum - upper[later_idx][column_idx] * weights[later_idx]
        weights[column_idx] = accum / upper[column_idx][column_idx]
    return weights


def last_body(recv_ref, q0_ref, q1_ref, w1_ref, old_ref, out_ref):
    vectors, length = q0_ref.shape
    beta, g00, h00, h10, g01, g11, h01, h11, h21 = get_scalars(old_ref, 9)
    h02, h12, h22, norm, g02, g12, g22 = unpack_dots(recv_ref[:, 0, :], 7, vectors)
    rest = (
        norm - 2.0 * (h02 * h02 + h12 * h12 + h22 * h22)
        + (h02 * h02 * g00 + h12 * h12 * g11 + h22 * h22 * g22)
        + 2.0 * (h02 * h12 * g01 + h02 * h22 * g02 + h12 * h22 * g12)
    )
    h32 = jnp.sqrt(jnp.maximum(rest, 0.0) + EPSILON)
    y0, y1, y2 = least_squares([[h00, h10], [h01, h11, h21], [h02, h12, h22, h32]], beta)
    q0 = q0_ref[...]
    q1 = q1_ref[...]
    q2 = (w1_ref[...] - h01 * q0 - h11 * q1) * (1.0 / h21)
    out_ref[...] = y0 * q0 + y1 * q1 + y2 * q2


def call(body, outs, args, scratch=(), flops=0, limit=20000, name=None):
    spaces = dict(s=pltpu.SMEM, v=pltpu.VMEM, h=pltpu.HBM)
    total = sum(math.prod(a.shape) * a.dtype.itemsize for _, a in list(args) + list(outs))
    return pl.pallas_call(
        body,
        out_shape=[pltpu.HBM(a.shape, a.dtype) if m == "h" else a for m, a in outs],
        in_specs=[pl.BlockSpec(memory_space=spaces[m]) for m, _ in args],
        out_specs=[pl.BlockSpec(memory_space=spaces[m]) for m, _ in outs],
        scratch_shapes=list(scratch),
        compiler_params=pltpu.CompilerParams(vmem_limit_bytes=limit * 1024),
        cost_estimate=pl.CostEstimate(flops=flops, bytes_accessed=total, transcendentals=0),
        name=name,
    )(*[pltpu.with_memory_space_constraint(a, pltpu.HBM) if m == "h" else a for m, a in args])


def exchange(payload):
    return lax.all_to_all(payload, AXES, 0, 0, tiled=True)


def per_device(
    coordinates, rhs, leaf_order, leaf_sizes, inverse_scales, noise_var, u_factors, v_factors
):
    vectors, length = rhs.shape
    dims = coordinates.shape[0]
    levels, rank, _ = u_factors.shape
    num = lax.axis_size("gx") * lax.axis_size("gy")
    blocks = length // TILE
    packed = TILE * (blocks * (blocks + 1) // 2)
    padded = dims // 8 * 8 + 8
    u_flat = u_factors.reshape(levels * rank, length)
    v_flat = v_factors.reshape(levels * rank, length)

    def shaped(*shape, dtype=f32):
        return jax.ShapeDtypeStruct(shape, dtype)

    field = ("v", shaped(vectors, length))
    factor = shaped(levels * rank, length, dtype=bf16)
    scalars = ("v", shaped(vectors, LANES))
    message = ("v", shaped(num, 1, rank * vectors + LANES))
    panel = shaped(packed // LANES * TILE, LANES, dtype=bf16)
    acc = pltpu.VMEM((3 * vectors, length), f32)
    panel_space = pltpu.VMEM((packed // LANES * TILE, LANES), bf16)
    whole_space = pltpu.VMEM((levels * rank, length), f32)
    sizes = dict(levels=levels, rank=rank)
    small = 2 * levels * rank * length * 256

    def arrays(memory, *values):
        return [(memory, value) for value in values]

    start, points, pay = call(
        functools.partial(start_body, **sizes),
        [field, ("v", shaped(padded, length)), message],
        arrays("s", leaf_sizes, noise_var)
        + arrays("h", inverse_scales, leaf_order, rhs, coordinates, v_flat),
        scratch=[
            pltpu.SMEM((dims,), f32),
            pltpu.VMEM((1, length), jnp.int32),
            pltpu.VMEM((vectors, length), f32),
            pltpu.VMEM((dims, length), f32),
            pltpu.VMEM((padded, length), f32),
            whole_space,
            pltpu.SemaphoreType.DMA((5,)),
        ],
        flops=small, name="start",
    )
    recv = exchange(pay)
    k1, k2, image, u1, u2 = call(
        functools.partial(build_body, dims=dims),
        [("h", panel), ("h", panel), field, ("v", factor), ("v", factor)],
        arrays("s", leaf_sizes) + arrays("v", points, start) + arrays("h", u_flat),
        scratch=[
            whole_space,
            pltpu.VMEM((dims, length, LANES), f32),
            panel_space,
            panel_space,
            acc,
            pltpu.SemaphoreType.DMA((1 + 2 * blocks,)),
        ],
        flops=2 * length * length * 256, limit=40000, name="build",
    )

    def near(vector, name):
        (out,) = call(
            functools.partial(near_body, dims=dims), [field],
            arrays("s", leaf_sizes) + arrays("v", points, vector)
            + arrays("h", k1, k2),
            scratch=[
                panel_space,
                panel_space,
                acc,
                pltpu.SemaphoreType.DMA((2 * blocks,)),
            ],
            flops=2 * length * length * 128, limit=30000, name=name,
        )
        return out

    whole_load = [whole_space, pltpu.SemaphoreType.DMA((1,))]
    q0, w0, scal, pay = call(
        functools.partial(first_body, **sizes),
        [field, field, scalars, message],
        arrays("s", leaf_sizes) + arrays("v", recv, image, start, u1, u2) + arrays("h", v_flat),
        scratch=whole_load, flops=small, name="first",
    )
    recv = exchange(pay)
    image = near(w0, "near1")
    q1, w1, scal, pay = call(
        functools.partial(second_body, **sizes),
        [field, field, scalars, message],
        arrays("s", leaf_sizes) + arrays("v", recv, image, q0, w0, scal, u1, u2)
        + arrays("h", v_flat),
        scratch=whole_load, flops=small, name="second",
    )
    recv = exchange(pay)
    image = near(w1, "near2")
    scal, pay = call(
        functools.partial(third_body, **sizes),
        [scalars, ("v", shaped(num, 1, LANES))],
        arrays("s", leaf_sizes) + arrays("v", recv, image, q0, q1, w0, w1, scal, u1, u2),
        flops=small, name="third",
    )
    recv = exchange(pay)
    placed = call(
        place_body, [field] * 3, arrays("v", leaf_order, q0, q1, w1),
        scratch=[pltpu.VMEM((9 * vectors, length), f32)],
        flops=2 * length * length * 128, name="place",
    )
    (out,) = call(
        last_body, [field], arrays("v", recv, *placed, scal), flops=small, name="last"
    )
    return out


def solution(mesh):
    in_specs = (
        P(None, AXES),
        P(None, AXES),
        P(AXES, None),
        P(AXES),
        P(),
        P(),
        P(None, None, AXES),
        P(None, None, AXES),
    )
    return jax.shard_map(
        per_device, mesh=mesh, in_specs=in_specs, out_specs=P(None, AXES), check_vma=False
    )
```

```python
import functools
import math

import jax
import jax.numpy as jnp
from jax import lax
from jax.experimental import pallas as pl
from jax.experimental.pallas import tpu as pltpu
from jax.sharding import PartitionSpec as P

AXES = ("gx", "gy")
LANES = 128
TILE = 256
EPSILON = 1e-06
DISTANCE_SCALE = math.sqrt(3.0) / math.log(2.0)
LN2 = math.log(2.0)
f32 = jnp.float32
bf16 = jnp.bfloat16


def split(x, parts):
    pieces = []
    for part in range(parts):
        piece = x.astype(bf16)
        pieces.append(piece)
        if part + 1 < parts:
            x = x - piece.astype(f32)
    return pieces


def dot(a, b):
    return lax.dot_general(a, b, (((1,), (0,)), ((), ())), preferred_element_type=f32)


def dot_nt(a, b):
    return lax.dot_general(a, b, (((1,), (1,)), ((), ())), preferred_element_type=f32)


def dot_halves(a, high, low):
    return dot(jnp.concatenate([a, a], axis=1), jnp.concatenate([high, low], axis=0))


def live_row(size, length):
    return lax.broadcasted_iota(jnp.int32, (1, length), 1) < size


def levels_of(num, levels):
    me = lax.axis_index("gx") * lax.axis_size("gy") + lax.axis_index("gy")
    apart = lax.broadcasted_iota(jnp.int32, (num, 1), 0) ^ me
    level = jnp.full((num, 1), -1, jnp.int32)
    for bit in range(levels):
        level = level + (apart >= (1 << bit)).astype(jnp.int32)
    return level


def diagonal(vectors):
    shape = (LANES // vectors, LANES)
    return lax.broadcasted_iota(jnp.int32, shape, 1) // vectors == lax.broadcasted_iota(
        jnp.int32, shape, 0
    )


def slot_mask(vectors, slot):
    shape = (vectors, LANES)
    return (
        lax.broadcasted_iota(jnp.int32, shape, 1)
        == lax.broadcasted_iota(jnp.int32, shape, 0) + slot * vectors
    )


def pack_dots(pairs, vectors):
    rows = jnp.zeros((vectors, LANES), f32)
    for slot, (a, b) in enumerate(pairs):
        total = jnp.sum(a * b, axis=1, keepdims=True)
        rows = jnp.where(slot_mask(vectors, slot), total, rows)
    return jnp.sum(rows, axis=0, keepdims=True)


def unpack_dots(received, count, vectors):
    total = jnp.sum(received, axis=0, keepdims=True)
    out = []
    for slot in range(count):
        chosen = jnp.where(slot_mask(vectors, slot), total, 0.0)
        out.append(jnp.sum(chosen, axis=1, keepdims=True))
    return out


def send_coefs(vector, high, low, pay_ref, dots, levels, rank):
    vectors = vector.shape[0]
    group = LANES // vectors
    num = pay_ref.shape[0]
    first, second = split(vector, 2)
    wide = jnp.concatenate([first] * group + [second] * group, axis=0)
    both = dot_nt(high, wide) + dot_nt(low, wide)
    both = both[:, :LANES] + both[:, LANES:]
    mask = diagonal(vectors)
    level = levels_of(num, levels)
    for block in range(rank // group):
        rows = jnp.zeros((num, LANES), f32)
        for lev in range(levels):
            start = lev * rank + block * group
            piece = jnp.where(mask, both[start : start + group], 0.0)
            rows = jnp.where(level == lev, jnp.sum(piece, axis=0, keepdims=True), rows)
        pay_ref[:, 0, block * LANES : (block + 1) * LANES] = rows
    pay_ref[:, 0, rank * vectors :] = jnp.broadcast_to(dots, (num, LANES))


def receive_coefs(recv_ref, vectors, levels, rank):
    num = recv_ref.shape[0]
    group = LANES // vectors
    mask = diagonal(vectors)
    level = levels_of(num, levels)
    pieces = []
    for lev in range(levels):
        for block in range(rank // group):
            part = recv_ref[:, 0, block * LANES : (block + 1) * LANES]
            total = jnp.sum(jnp.where(level == lev, part, 0.0), axis=0, keepdims=True)
            pieces.append(jnp.where(mask, jnp.broadcast_to(total, mask.shape), 0.0))
    flipped = jnp.concatenate(pieces, axis=0).T
    out = flipped[:vectors]
    for row in range(1, group):
        out = out + flipped[row * vectors : (row + 1) * vectors]
    return out


def expand(coefs, high, low):
    vectors = coefs.shape[0]
    stacked = jnp.concatenate(split(coefs, 3), axis=0)
    out = dot(stacked, high) + dot(stacked, low)
    return out[:vectors] + out[vectors : 2 * vectors] + out[2 * vectors :]


def one_hot(row, length):
    width = row.shape[1]
    steps = lax.broadcasted_iota(jnp.int32, (TILE, width), 0).astype(f32).astype(bf16)
    pieces = []
    for base in range(0, length, TILE):
        local = (row - base).astype(f32)
        local = jnp.broadcast_to(local, (TILE, width)).astype(bf16)
        pieces.append(jnp.where(steps == local, jnp.ones((), bf16), jnp.zeros((), bf16)))
    return jnp.concatenate(pieces, axis=0)


def start_body(
    sizes_ref, noise_ref, scales_hbm, order_hbm, rhs_hbm, coords_hbm, v_hbm,
    start_ref, points_ref, pay_ref,
    scales_ref, order_ref, rhs_ref, coords_ref, pad_ref, v_ref, sem, *, levels, rank,
):
    loads = [
        pltpu.make_async_copy(source, target, sem.at[n])
        for n, (source, target) in enumerate(
            [
                (scales_hbm, scales_ref),
                (order_hbm, order_ref),
                (rhs_hbm, rhs_ref),
                (coords_hbm, coords_ref),
                (v_hbm, v_ref),
            ]
        )
    ]
    for load in loads:
        load.start()
    vectors, length = rhs_ref.shape
    dims = coords_ref.shape[0]
    pad_ref[...] = jnp.zeros(pad_ref.shape, f32)
    for load in loads[:4]:
        load.wait()
    pad_ref[:dims, :] = coords_ref[...]
    stacked = jnp.concatenate(
        [p.astype(f32) for p in split(rhs_ref[...], 3)]
        + [p.astype(f32) for p in split(pad_ref[...], 3)],
        axis=0,
    ).astype(bf16)
    rows = pad_ref.shape[0]
    row_id = lax.broadcasted_iota(jnp.int32, (rows, 1), 0)
    scale = jnp.zeros((rows, 1), f32)
    for dim in range(dims):
        scale = jnp.where(row_id == dim, scales_ref[dim] * DISTANCE_SCALE, scale)
    for base in range(0, length, TILE):
        chosen = dot(stacked, one_hot(order_ref[:, base : base + TILE], length))
        lane = base + lax.broadcasted_iota(jnp.int32, (1, TILE), 1)
        value = chosen[:vectors] + chosen[vectors : 2 * vectors] + chosen[2 * vectors : 3 * vectors]
        start_ref[:, base : base + TILE] = jnp.where(lane < sizes_ref[0], value, 0.0)
        rest = chosen[3 * vectors :]
        value = rest[:rows] + rest[rows : 2 * rows] + rest[2 * rows :]
        points_ref[:, base : base + TILE] = jnp.where(row_id == dims, noise_ref[0], value * scale)

    @stage(sizes_ref[0])
    def _():
        loads[4].wait()
        high, low = split(v_ref[...], 2)
        start = start_ref[...]
        dots = pack_dots([(start, start)], vectors)
        send_coefs(start, high, low, pay_ref, dots, levels, rank)


def blocks_of(ref, first, count):
    return jnp.concatenate(
        [ref[(first + n) * TILE : (first + n + 1) * TILE, :] for n in range(count)], axis=1
    )


def stage(value):
    return pl.when(value > -1)


def add_panel(stacked, high_ref, low_ref, acc_ref, base, offset):
    width = acc_ref.shape[1] - base
    own = stacked[:, base : base + TILE]
    first = offset // LANES
    high = blocks_of(high_ref, first, width // LANES)
    low = blocks_of(low_ref, first, width // LANES)
    acc_ref[:, base:] += dot_halves(own, high, low)
    if width > TILE:
        rest = stacked[:, base + TILE :]
        acc_ref[:, base : base + TILE] += dot_nt(
            jnp.concatenate([rest, rest], axis=1),
            jnp.concatenate([high[:, TILE:], low[:, TILE:]], axis=1),
        )


def panel_rows(ref, offset, width):
    return ref.at[pl.ds(offset // LANES * TILE, width // LANES * TILE), :]


def finish(acc_ref, points_ref, vector, dims):
    vectors = vector.shape[0]
    out = acc_ref[...]
    out = out[:vectors] + out[vectors : 2 * vectors] + out[2 * vectors :]
    return LN2 * out + points_ref[dims : dims + 1, :] * vector


def panels(length):
    offset = 0
    for base in range(0, length, TILE):
        yield base, offset, length - base
        offset += length - base


def build_body(
    sizes_ref, points_ref, start_ref, u_hbm, high_hbm, low_hbm, image_ref, u1_ref, u2_ref,
    u_ref, wide_ref, high_ref, low_ref, acc_ref, sem, *, dims,
):
    length = points_ref.shape[1]
    step = 16
    load = pltpu.make_async_copy(u_hbm, u_ref, sem.at[0])
    load.start()
    columns = points_ref[...].T
    for dim in range(dims):
        wide_ref[dim] = jnp.broadcast_to(columns[:, dim : dim + 1], (length, LANES))
    start = start_ref[...]
    stacked = jnp.concatenate(split(start, 3), axis=0)
    acc_ref[...] = jnp.zeros(acc_ref.shape, f32)
    copies = []
    for base, offset, width in panels(length):
        for row in range(0, TILE, step):
            column = [wide_ref[dim, base + row : base + row + step, :] for dim in range(dims)]
            for lane in range(base, length, LANES):
                square = None
                for dim in range(dims):
                    differ = column[dim] - points_ref[dim : dim + 1, lane : lane + LANES]
                    square = differ * differ if square is None else square + differ * differ
                square = jnp.maximum(square, 1e-30)
                distance = square * lax.rsqrt(square)
                value = (1.0 / LN2 + distance) * jnp.exp2(-distance)
                high, low = split(value, 2)
                place = (offset + lane - base) // LANES * TILE + row
                high_ref[place : place + step, :] = high
                low_ref[place : place + step, :] = low
        for source, target in ((high_ref, high_hbm), (low_ref, low_hbm)):
            copy = pltpu.make_async_copy(
                panel_rows(source, offset, width),
                panel_rows(target, offset, width),
                sem.at[1 + len(copies)],
            )
            copy.start()
            copies.append(copy)
        add_panel(stacked, high_ref, low_ref, acc_ref, base, offset)

    @stage(sizes_ref[0])
    def _():
        image_ref[...] = finish(acc_ref, points_ref, start, dims)
        load.wait()
        high, low = split(u_ref[...], 2)
        u1_ref[...] = high
        u2_ref[...] = low

    @stage(sizes_ref[0])
    def _():
        for copy in copies:
            copy.wait()


def near_body(
    sizes_ref, points_ref, vector_ref, high_hbm, low_hbm, image_ref,
    high_ref, low_ref, acc_ref, sem, *, dims,
):
    vector = vector_ref[...]
    length = vector.shape[1]
    copies = []
    for base, offset, width in panels(length):
        for source, target in ((high_hbm, high_ref), (low_hbm, low_ref)):
            copy = pltpu.make_async_copy(
                panel_rows(source, offset, width),
                panel_rows(target, offset, width),
                sem.at[len(copies)],
            )
            copies.append(copy)
    ahead = 6
    for copy in copies[:ahead]:
        copy.start()
    stacked = jnp.concatenate(split(vector, 3), axis=0)
    acc_ref[...] = jnp.zeros(acc_ref.shape, f32)
    for number, (base, offset, width) in enumerate(panels(length)):

        @stage(sizes_ref[0])
        def _(number=number, base=base, offset=offset):
            for copy in copies[2 * number : 2 * number + 2]:
                copy.wait()
            for copy in copies[2 * number + ahead : 2 * number + ahead + 2]:
                copy.start()
            add_panel(stacked, high_ref, low_ref, acc_ref, base, offset)

    @stage(sizes_ref[0])
    def _():
        image_ref[...] = finish(acc_ref, points_ref, vector, dims)


def place_body(order_ref, *refs):
    count = (len(refs) - 1) // 2
    sources, targets, acc_ref = refs[:count], refs[count : 2 * count], refs[-1]
    vectors, length = sources[0].shape
    stacked = jnp.concatenate([p for ref in sources for p in split(ref[...], 3)], axis=0)
    for base in range(0, length, TILE):
        hot = one_hot(order_ref[:, base : base + TILE], length)
        part = dot_nt(stacked[:, base : base + TILE], hot)
        if base == 0:
            acc_ref[...] = part
        else:
            acc_ref[...] += part
    for number, target in enumerate(targets):
        first = 3 * number * vectors
        pieces = [acc_ref[first + n * vectors : first + (n + 1) * vectors, :] for n in range(3)]
        target[...] = pieces[0] + pieces[1] + pieces[2]


def first_body(
    sizes_ref, recv_ref, image_ref, start_ref, u1_ref, u2_ref, v_hbm,
    q0_ref, w0_ref, scal_ref, pay_ref, v_ref, sem, *, levels, rank,
):
    load = pltpu.make_async_copy(v_hbm, v_ref, sem.at[0])
    load.start()
    vectors, length = start_ref.shape
    live = live_row(sizes_ref[0], length)
    (norm,) = unpack_dots(recv_ref[:, 0, rank * vectors :], 1, vectors)
    beta = jnp.sqrt(norm + EPSILON)
    inverse = 1.0 / beta
    distant = expand(receive_coefs(recv_ref, vectors, levels, rank), u1_ref[...], u2_ref[...])
    w0 = jnp.where(live, image_ref[...] + distant, 0.0) * inverse
    q0 = start_ref[...] * inverse
    q0_ref[...] = q0
    w0_ref[...] = w0
    scal_ref[...] = jnp.broadcast_to(beta, scal_ref.shape)
    dots = pack_dots([(q0, q0), (q0, w0), (w0, w0)], vectors)

    @stage(sizes_ref[0])
    def _():
        load.wait()
        high, low = split(v_ref[...], 2)
        send_coefs(w0_ref[...], high, low, pay_ref, dots, levels, rank)


def put_scalars(scal_ref, values):
    lane = lax.broadcasted_iota(jnp.int32, scal_ref.shape, 1)
    out = jnp.zeros(scal_ref.shape, f32)
    for slot, value in enumerate(values):
        out = jnp.where(lane == slot, value, out)
    scal_ref[...] = out


def get_scalars(scal_ref, count):
    return [scal_ref[:, slot : slot + 1] for slot in range(count)]


def second_body(
    sizes_ref, recv_ref, image_ref, q0_ref, w0_ref, old_ref, u1_ref, u2_ref, v_hbm,
    q1_ref, w1_ref, scal_ref, pay_ref, v_ref, sem, *, levels, rank,
):
    load = pltpu.make_async_copy(v_hbm, v_ref, sem.at[0])
    load.start()
    vectors, length = q0_ref.shape
    live = live_row(sizes_ref[0], length)
    (beta,) = get_scalars(old_ref, 1)
    g00, h00, norm = unpack_dots(recv_ref[:, 0, rank * vectors :], 3, vectors)
    rest = norm - 2.0 * h00 * h00 + h00 * h00 * g00
    h10 = jnp.sqrt(jnp.maximum(rest, 0.0) + EPSILON)
    inverse = 1.0 / h10
    put_scalars(scal_ref, [beta, g00, h00, h10])
    distant = expand(receive_coefs(recv_ref, vectors, levels, rank), u1_ref[...], u2_ref[...])
    w0 = w0_ref[...]
    q0 = q0_ref[...]
    q1 = (w0 - h00 * q0) * inverse
    w1 = (jnp.where(live, image_ref[...] + distant, 0.0) - h00 * w0) * inverse
    q1_ref[...] = q1
    w1_ref[...] = w1
    dots = pack_dots([(q0, w1), (q1, w1), (w1, w1), (q0, q1), (q1, q1)], vectors)

    @stage(sizes_ref[0])
    def _():
        load.wait()
        high, low = split(v_ref[...], 2)
        send_coefs(w1_ref[...], high, low, pay_ref, dots, levels, rank)


def third_body(
    sizes_ref, recv_ref, image_ref, q0_ref, q1_ref, w0_ref, w1_ref, old_ref, u1_ref, u2_ref,
    scal_ref, pay_ref, *, levels, rank,
):
    vectors, length = q0_ref.shape
    live = live_row(sizes_ref[0], length)
    beta, g00, h00, h10 = get_scalars(old_ref, 4)
    h01, h11, norm, g01, g11 = unpack_dots(recv_ref[:, 0, rank * vectors :], 5, vectors)
    rest = (
        norm - 2.0 * (h01 * h01 + h11 * h11)
        + (h01 * h01 * g00 + h11 * h11 * g11 + 2.0 * h01 * h11 * g01)
    )
    h21 = jnp.sqrt(jnp.maximum(rest, 0.0) + EPSILON)
    inverse = 1.0 / h21
    put_scalars(scal_ref, [beta, g00, h00, h10, g01, g11, h01, h11, h21])
    distant = expand(receive_coefs(recv_ref, vectors, levels, rank), u1_ref[...], u2_ref[...])
    w0 = w0_ref[...]
    w1 = w1_ref[...]
    q0 = q0_ref[...]
    q1 = q1_ref[...]
    q2 = (w1 - h01 * q0 - h11 * q1) * inverse
    image = jnp.where(live, image_ref[...] + distant, 0.0)
    w2 = (image - h01 * w0 - h11 * w1) * inverse
    dots = pack_dots(
        [(q0, w2), (q1, w2), (q2, w2), (w2, w2), (q0, q2), (q1, q2), (q2, q2)], vectors
    )
    num, _, width = pay_ref.shape
    pay_ref[:, 0, :] = jnp.broadcast_to(dots, (num, width))


def least_squares(columns, beta):
    count_cols = len(columns)
    cosines = []
    sines = []
    target = [beta] + [jnp.zeros_like(beta)] * count_cols
    upper = []
    for column_idx in range(count_cols):
        entries = list(columns[column_idx])
        for row_idx in range(column_idx):
            first_val = entries[row_idx]
            second_val = entries[row_idx + 1]
            entries[row_idx] = cosines[row_idx] * first_val + sines[row_idx] * second_val
            entries[row_idx + 1] = -sines[row_idx] * first_val + cosines[row_idx] * second_val
        first_val = entries[column_idx]
        second_val = entries[column_idx + 1]
        radius = jnp.sqrt(first_val * first_val + second_val * second_val)
        cosines.append(first_val / radius)
        sines.append(second_val / radius)
        entries[column_idx] = radius
        carried = target[column_idx]
        target[column_idx] = cosines[column_idx] * carried
        target[column_idx + 1] = -sines[column_idx] * carried
        upper.append(entries[: column_idx + 1])
    weights = [None] * count_cols
    for column_idx in reversed(range(count_cols)):
        accum = target[column_idx]
        for later_idx in range(column_idx + 1, count_cols):
            accum = accum - upper[later_idx][column_idx] * weights[later_idx]
        weights[column_idx] = accum / upper[column_idx][column_idx]
    return weights


def last_body(recv_ref, q0_ref, q1_ref, w1_ref, old_ref, out_ref):
    vectors, length = q0_ref.shape
    beta, g00, h00, h10, g01, g11, h01, h11, h21 = get_scalars(old_ref, 9)
    h02, h12, h22, norm, g02, g12, g22 = unpack_dots(recv_ref[:, 0, :], 7, vectors)
    rest = (
        norm - 2.0 * (h02 * h02 + h12 * h12 + h22 * h22)
        + (h02 * h02 * g00 + h12 * h12 * g11 + h22 * h22 * g22)
        + 2.0 * (h02 * h12 * g01 + h02 * h22 * g02 + h12 * h22 * g12)
    )
    h32 = jnp.sqrt(jnp.maximum(rest, 0.0) + EPSILON)
    y0, y1, y2 = least_squares([[h00, h10], [h01, h11, h21], [h02, h12, h22, h32]], beta)
    q0 = q0_ref[...]
    q1 = q1_ref[...]
    q2 = (w1_ref[...] - h01 * q0 - h11 * q1) * (1.0 / h21)
    out_ref[...] = y0 * q0 + y1 * q1 + y2 * q2


def call(body, outs, args, scratch=(), flops=0, limit=20000, name=None):
    spaces = dict(s=pltpu.SMEM, v=pltpu.VMEM, h=pltpu.HBM)
    total = sum(math.prod(a.shape) * a.dtype.itemsize for _, a in list(args) + list(outs))
    return pl.pallas_call(
        body,
        out_shape=[pltpu.HBM(a.shape, a.dtype) if m == "h" else a for m, a in outs],
        in_specs=[pl.BlockSpec(memory_space=spaces[m]) for m, _ in args],
        out_specs=[pl.BlockSpec(memory_space=spaces[m]) for m, _ in outs],
        scratch_shapes=list(scratch),
        compiler_params=pltpu.CompilerParams(vmem_limit_bytes=limit * 1024),
        cost_estimate=pl.CostEstimate(flops=flops, bytes_accessed=total, transcendentals=0),
        name=name,
    )(*[pltpu.with_memory_space_constraint(a, pltpu.HBM) if m == "h" else a for m, a in args])


def exchange(payload):
    return lax.all_to_all(payload, AXES, 0, 0, tiled=True)


def per_device(
    coordinates, rhs, leaf_order, leaf_sizes, inverse_scales, noise_var, u_factors, v_factors
):
    vectors, length = rhs.shape
    dims = coordinates.shape[0]
    levels, rank, _ = u_factors.shape
    num = lax.axis_size("gx") * lax.axis_size("gy")
    blocks = length // TILE
    packed = TILE * (blocks * (blocks + 1) // 2)
    padded = dims // 8 * 8 + 8
    u_flat = u_factors.reshape(levels * rank, length)
    v_flat = v_factors.reshape(levels * rank, length)

    def shaped(*shape, dtype=f32):
        return jax.ShapeDtypeStruct(shape, dtype)

    field = ("v", shaped(vectors, length))
    factor = shaped(levels * rank, length, dtype=bf16)
    scalars = ("v", shaped(vectors, LANES))
    message = ("v", shaped(num, 1, rank * vectors + LANES))
    panel = shaped(packed // LANES * TILE, LANES, dtype=bf16)
    acc = pltpu.VMEM((3 * vectors, length), f32)
    panel_space = pltpu.VMEM((packed // LANES * TILE, LANES), bf16)
    whole_space = pltpu.VMEM((levels * rank, length), f32)
    sizes = dict(levels=levels, rank=rank)
    small = 2 * levels * rank * length * 256

    def arrays(memory, *values):
        return [(memory, value) for value in values]

    start, points, pay = call(
        functools.partial(start_body, **sizes),
        [field, ("v", shaped(padded, length)), message],
        arrays("s", leaf_sizes, noise_var)
        + arrays("h", inverse_scales, leaf_order, rhs, coordinates, v_flat),
        scratch=[
            pltpu.SMEM((dims,), f32),
            pltpu.VMEM((1, length), jnp.int32),
            pltpu.VMEM((vectors, length), f32),
            pltpu.VMEM((dims, length), f32),
            pltpu.VMEM((padded, length), f32),
            whole_space,
            pltpu.SemaphoreType.DMA((5,)),
        ],
        flops=small, name="start",
    )
    recv = exchange(pay)
    k1, k2, image, u1, u2 = call(
        functools.partial(build_body, dims=dims),
        [("h", panel), ("h", panel), field, ("v", factor), ("v", factor)],
        arrays("s", leaf_sizes) + arrays("v", points, start) + arrays("h", u_flat),
        scratch=[
            whole_space,
            pltpu.VMEM((dims, length, LANES), f32),
            panel_space,
            panel_space,
            acc,
            pltpu.SemaphoreType.DMA((1 + 2 * blocks,)),
        ],
        flops=2 * length * length * 256, limit=40000, name="build",
    )

    def near(vector, name):
        (out,) = call(
            functools.partial(near_body, dims=dims), [field],
            arrays("s", leaf_sizes) + arrays("v", points, vector)
            + arrays("h", k1, k2),
            scratch=[
                panel_space,
                panel_space,
                acc,
                pltpu.SemaphoreType.DMA((2 * blocks,)),
            ],
            flops=2 * length * length * 128, limit=30000, name=name,
        )
        return out

    whole_load = [whole_space, pltpu.SemaphoreType.DMA((1,))]
    q0, w0, scal, pay = call(
        functools.partial(first_body, **sizes),
        [field, field, scalars, message],
        arrays("s", leaf_sizes) + arrays("v", recv, image, start, u1, u2) + arrays("h", v_flat),
        scratch=whole_load, flops=small, name="first",
    )
    recv = exchange(pay)
    image = near(w0, "near1")
    q1, w1, scal, pay = call(
        functools.partial(second_body, **sizes),
        [field, field, scalars, message],
        arrays("s", leaf_sizes) + arrays("v", recv, image, q0, w0, scal, u1, u2)
        + arrays("h", v_flat),
        scratch=whole_load, flops=small, name="second",
    )
    recv = exchange(pay)
    image = near(w1, "near2")
    scal, pay = call(
        functools.partial(third_body, **sizes),
        [scalars, ("v", shaped(num, 1, LANES))],
        arrays("s", leaf_sizes) + arrays("v", recv, image, q0, q1, w0, w1, scal, u1, u2),
        flops=small, name="third",
    )
    recv = exchange(pay)
    placed = call(
        place_body, [field] * 3, arrays("v", leaf_order, q0, q1, w1),
        scratch=[pltpu.VMEM((9 * vectors, length), f32)],
        flops=2 * length * length * 128, name="place",
    )
    (out,) = call(
        last_body, [field], arrays("v", recv, *placed, scal), flops=small, name="last"
    )
    return out


def solution(mesh):
    in_specs = (
        P(None, AXES),
        P(None, AXES),
        P(AXES, None),
        P(AXES),
        P(),
        P(),
        P(None, None, AXES),
        P(None, None, AXES),
    )
    return jax.shard_map(
        per_device, mesh=mesh, in_specs=in_specs, out_specs=P(None, AXES), check_vma=False
    )
```
